32 devices in a mesh: dp: 32 (over z, y, x, core).
Axes of the slice: x: 2, y: 2, z: 4, core: 2. Of those that a mesh axis runs over, the one named last changes fastest.
Arguments:
- x_rows: bfloat16 [131072, 576], P('dp')
- dy_rows: bfloat16 [131072, 576], P('dp')
- w_one: bfloat16 [576, 6144], replicated
- w_two: bfloat16 [6144, 576], replicated
- w_three: bfloat16 [576, 1536], replicated
- w_four: bfloat16 [1536, 576], replicated
- master_one: float32 [576, 6144], P('dp')
- master_two: float32 [6144, 576], P('dp')
- master_three: float32 [576, 1536], P('dp')
- master_four: float32 [1536, 576], P('dp')
- m_one: float32 [576, 6144], P('dp')
- m_two: float32 [6144, 576], P('dp')
- m_three: float32 [576, 1536], P('dp')
- m_four: float32 [1536, 576], P('dp')
- v_one: float32 [576, 6144], P('dp')
- v_two: float32 [6144, 576], P('dp')
- v_three: float32 [576, 1536], P('dp')
- v_four: float32 [1536, 576], P('dp')
- learn_rate: float32 [], replicated
- clip_max: float32 [], replicated
Outputs:
- output 1: bfloat16 [576, 6144], replicated
- output 2: bfloat16 [6144, 576], replicated
- output 3: bfloat16 [576, 1536], replicated
- output 4: bfloat16 [1536, 576], replicated
- output 5: float32 [576, 6144], P('dp')
- output 6: float32 [6144, 576], P('dp')
- output 7: float32 [576, 1536], P('dp')
- output 8: float32 [1536, 576], P('dp')
- output 9: float32 [576, 6144], P('dp')
- output 10: float32 [6144, 576], P('dp')
- output 11: float32 [576, 1536], P('dp')
- output 12: float32 [1536, 576], P('dp')
- output 13: float32 [576, 6144], P('dp')
- output 14: float32 [6144, 576], P('dp')
- output 15: float32 [576, 1536], P('dp')
- output 16: float32 [1536, 576], P('dp')
- output 17: float32 [], replicated
All inputs are finite; a program needn't handle non-finite values.
Results may differ from the reference program's by a relative error of at most 0.0126751.
Values are sent between devices in bfloat16 or wider.
A program may use at most 1 GiB of HBM per device.

```python
import math
import jax
import jax.numpy as jnp
from jax import lax

MODEL_DIM = 576
FF_DIM = 1536
ROWS_DEV = 4096
DP_SIZE = 32
ADAM_STEP = 10
WIDE_DIM = 4 * FF_DIM
BETA_ONE = 0.9
BETA_TWO = 0.95
ADAM_EPS = 1e-8
NORM_EPS = 1e-6
BIAS_ONE = 1.0 - BETA_ONE ** ADAM_STEP
BIAS_TWO = 1.0 - BETA_TWO ** ADAM_STEP
INV_SQRT2 = 0.7071067811865476
INV_SQRT2PI = 0.3989422804014327
STD_ONE = 1.0 / (1.5 * math.sqrt(MODEL_DIM))
STD_TWO = math.sqrt(2.0 / 0.43) / math.sqrt(WIDE_DIM)
STD_THREE = 1.0 / math.sqrt(2.0 * MODEL_DIM)
STD_FOUR = 1.0 / math.sqrt(0.43 * FF_DIM)


def gelu_value(pre_act):
    pre_wide = pre_act.astype(jnp.float32)
    return 0.5 * pre_wide * (1.0 + lax.erf(pre_wide * INV_SQRT2))


def gelu_slope(pre_act):
    pre_wide = pre_act.astype(jnp.float32)
    return 0.5 * (1.0 + lax.erf(pre_wide * INV_SQRT2)) + pre_wide * INV_SQRT2PI * jnp.exp(-0.5 * pre_wide * pre_wide)


def local_grads(x_rows, dy_rows, w_one, w_two, w_three, w_four):
    z_one = jnp.dot(x_rows, w_one, preferred_element_type=jnp.float32).astype(jnp.bfloat16)
    a_one = gelu_value(z_one).astype(jnp.bfloat16)
    h_two = jnp.dot(a_one, w_two, preferred_element_type=jnp.float32).astype(jnp.bfloat16)
    z_three = jnp.dot(h_two, w_three, preferred_element_type=jnp.float32).astype(jnp.bfloat16)
    a_three = gelu_value(z_three).astype(jnp.bfloat16)
    g_four = jnp.dot(a_three.T, dy_rows, preferred_element_type=jnp.float32)
    da_three = jnp.dot(dy_rows, w_four.T, preferred_element_type=jnp.float32).astype(jnp.bfloat16)
    dz_three = (da_three.astype(jnp.float32) * gelu_slope(z_three)).astype(jnp.bfloat16)
    g_three = jnp.dot(h_two.T, dz_three, preferred_element_type=jnp.float32)
    dh_two = jnp.dot(dz_three, w_three.T, preferred_element_type=jnp.float32).astype(jnp.bfloat16)
    g_two = jnp.dot(a_one.T, dh_two, preferred_element_type=jnp.float32)
    da_one = jnp.dot(dh_two, w_two.T, preferred_element_type=jnp.float32).astype(jnp.bfloat16)
    dz_one = (da_one.astype(jnp.float32) * gelu_slope(z_one)).astype(jnp.bfloat16)
    g_one = jnp.dot(x_rows.T, dz_one, preferred_element_type=jnp.float32)
    return g_one, g_two, g_three, g_four


def mean_grads(x_rows, dy_rows, w_one, w_two, w_three, w_four):
    x_parts = x_rows.reshape(DP_SIZE, ROWS_DEV, MODEL_DIM)
    dy_parts = dy_rows.reshape(DP_SIZE, ROWS_DEV, MODEL_DIM)
    zero_sums = (jnp.zeros((MODEL_DIM, WIDE_DIM), jnp.float32), jnp.zeros((WIDE_DIM, MODEL_DIM), jnp.float32), jnp.zeros((MODEL_DIM, FF_DIM), jnp.float32), jnp.zeros((FF_DIM, MODEL_DIM), jnp.float32))

    def add_part(running, part_pair):
        part_grads = local_grads(part_pair[0], part_pair[1], w_one, w_two, w_three, w_four)
        return tuple(run_sum + new_grad for run_sum, new_grad in zip(running, part_grads)), None

    grad_sums, _unused = lax.scan(add_part, zero_sums, (x_parts, dy_parts))
    return tuple(grad_sum / DP_SIZE for grad_sum in grad_sums)


def adam_rows(grad_mat, master_mat, mom_mat, var_mat, clip_scale, learn_rate):
    scaled = clip_scale * grad_mat
    mom_new = BETA_ONE * mom_mat + (1.0 - BETA_ONE) * scaled
    var_new = BETA_TWO * var_mat + (1.0 - BETA_TWO) * scaled * scaled
    master_new = master_mat - learn_rate * (mom_new / BIAS_ONE) / (jnp.sqrt(var_new / BIAS_TWO) + ADAM_EPS)
    return master_new, mom_new, var_new


def setup_inputs(seed: int = 0) -> dict:
    key_list = jax.random.split(jax.random.key(seed), 16)
    batch_rows = DP_SIZE * ROWS_DEV
    x_rows = (1.5 * jax.random.normal(key_list[0], (batch_rows, MODEL_DIM), jnp.float32)).astype(jnp.bfloat16)
    dy_rows = jax.random.normal(key_list[1], (batch_rows, MODEL_DIM), jnp.float32).astype(jnp.bfloat16)
    shape_list = ((MODEL_DIM, WIDE_DIM), (WIDE_DIM, MODEL_DIM), (MODEL_DIM, FF_DIM), (FF_DIM, MODEL_DIM))
    std_list = (STD_ONE, STD_TWO, STD_THREE, STD_FOUR)
    masters = [std_val * jax.random.normal(key_list[2 + mat_index], shape_list[mat_index], jnp.float32) for mat_index, std_val in enumerate(std_list)]
    weights = [master_mat.astype(jnp.bfloat16) for master_mat in masters]
    grads = mean_grads(x_rows, dy_rows, weights[0], weights[1], weights[2], weights[3])
    grad_norm = jnp.sqrt(sum(jnp.sum(grad_mat * grad_mat) for grad_mat in grads))
    clip_frac = jax.random.uniform(key_list[6], (), jnp.float32, minval=0.3, maxval=0.7)
    clip_max = clip_frac * grad_norm
    learn_rate = jax.random.uniform(key_list[7], (), jnp.float32, minval=0.5, maxval=1.5) / math.sqrt(MODEL_DIM)
    mom_list = []
    var_list = []
    for mat_index, grad_mat in enumerate(grads):
        grad_rms = clip_frac * jnp.sqrt(jnp.mean(grad_mat * grad_mat))
        mom_list.append(0.1 * grad_rms * jax.random.normal(key_list[8 + mat_index], shape_list[mat_index], jnp.float32))
        var_list.append(grad_rms * grad_rms * jax.random.uniform(key_list[12 + mat_index], shape_list[mat_index], jnp.float32, minval=0.5, maxval=1.5))
    return {'x_rows': x_rows, 'dy_rows': dy_rows, 'w_one': weights[0], 'w_two': weights[1], 'w_three': weights[2], 'w_four': weights[3], 'master_one': masters[0], 'master_two': masters[1], 'master_three': masters[2], 'master_four': masters[3], 'm_one': mom_list[0], 'm_two': mom_list[1], 'm_three': mom_list[2], 'm_four': mom_list[3], 'v_one': var_list[0], 'v_two': var_list[1], 'v_three': var_list[2], 'v_four': var_list[3], 'learn_rate': learn_rate, 'clip_max': clip_max}


def reference(x_rows, dy_rows, w_one, w_two, w_three, w_four, master_one, master_two, master_three, master_four, m_one, m_two, m_three, m_four, v_one, v_two, v_three, v_four, learn_rate, clip_max):
    grads = mean_grads(x_rows, dy_rows, w_one, w_two, w_three, w_four)
    grad_norm = jnp.sqrt(sum(jnp.sum(grad_mat * grad_mat) for grad_mat in grads))
    clip_scale = jnp.minimum(1.0, clip_max / (grad_norm + NORM_EPS))
    res_one = adam_rows(grads[0], master_one, m_one, v_one, clip_scale, learn_rate)
    res_two = adam_rows(grads[1], master_two, m_two, v_two, clip_scale, learn_rate)
    res_three = adam_rows(grads[2], master_three, m_three, v_three, clip_scale, learn_rate)
    res_four = adam_rows(grads[3], master_four, m_four, v_four, clip_scale, learn_rate)
    return (res_one[0].astype(jnp.bfloat16), res_two[0].astype(jnp.bfloat16), res_three[0].astype(jnp.bfloat16), res_four[0].astype(jnp.bfloat16), res_one[0], res_two[0], res_three[0], res_four[0], res_one[1], res_two[1], res_three[1], res_four[1], res_one[2], res_two[2], res_three[2], res_four[2], grad_norm)
```

```python
import functools
import jax
import jax.numpy as jnp
from jax import lax
from jax.experimental import pallas as pl
from jax.experimental.pallas import tpu as pltpu
from jax.sharding import PartitionSpec as P

ADAM_STEP = 10
BETA_ONE = 0.9
BETA_TWO = 0.95
ADAM_EPS = 1e-8
NORM_EPS = 1e-6
BIAS_ONE = 1.0 - BETA_ONE ** ADAM_STEP
BIAS_TWO = 1.0 - BETA_TWO ** ADAM_STEP
INV_SQRT2 = 0.7071067811865476
INV_SQRT2PI = 0.3989422804014327
DP_SIZE = 32
MESH_ID = pl.DeviceIdType.MESH
W1_ROWS = 48 * 18
W3_ROWS = 12 * 18
PACK_ROWS = 1088
CHUNKS = 12
CHUNK_W = 512
ROWS_DEV = 4096
TILE_R = 512
LANES = 128
MODEL_DIM = 576
GROUP_ROWS = 72
HALF_ROWS = 288
OWN_ROWS = 18
Z_SIZE = 4
PAIR = 2
Z_PEERS = 3
PAD_ROWS = 24
WIDE_DIM = 6144
FF_DIM = 1536
STACK_ROWS = 240
TALL_ROWS = 192
SHORT_ROWS = 48


def gelu_value(pre_act):
    pre_wide = pre_act.astype(jnp.float32)
    return 0.5 * pre_wide * (1.0 + lax.erf(pre_wide * INV_SQRT2))


def device_of(core, x_pos, y_pos, z_pos):
    return ((z_pos * PAIR + y_pos) * PAIR + x_pos) * PAIR + core


def update_kernel(g1, g2, g3, g4, p1, p2, p3, p4, m1, m2, m3, m4, v1, v2, v3, v4, lr_ref, clip_ref,
                  all_p, all_q, p1n, p2n, p3n, p4n, m1n, m2n, m3n, m4n, v1n, v2n, v3n, v4n, norm_ref,
                  wide_p, own_p, own_q, norm_send, norm_recv,
                  norm_ssem, norm_rsem, send_p, recv_p, send_q, recv_q, local_sem):
    me = lax.axis_index('dp')
    core = me % PAIR
    x_pos = (me // PAIR) % PAIR
    y_pos = (me // Z_SIZE) % PAIR
    z_pos = me // 8
    core_peer = device_of(1 - core, x_pos, y_pos, z_pos)
    x_peer = device_of(core, 1 - x_pos, y_pos, z_pos)
    y_peer = device_of(core, x_pos, 1 - y_pos, z_pos)
    z_others = [(z_pos + k) % Z_SIZE for k in (1, PAIR, Z_PEERS)]
    z_peers = [device_of(core, x_pos, y_pos, zo) for zo in z_others]

    barrier = pltpu.get_barrier_semaphore()
    for peer in [core_peer, x_peer, y_peer] + z_peers:
        pl.semaphore_signal(barrier, inc=1, device_id=(peer,), device_id_type=MESH_ID)
    pl.semaphore_wait(barrier, 6)

    inv_dp = 1.0 / DP_SIZE
    total = jnp.zeros((1, LANES), jnp.float32)
    for g_ref in (g1, g3):
        for j in range(g_ref.shape[1] // LANES):
            g_val = g_ref[:, j * LANES:(j + 1) * LANES] * inv_dp
            total = total + jnp.sum(g_val * g_val, axis=0, keepdims=True)
    scal = jnp.sum(total)
    for g_ref in (g2, g4):
        g_val = g_ref[...] * inv_dp
        scal = scal + jnp.sum(g_val * g_val)
    part = jnp.full((8, LANES), scal, jnp.float32)
    for stage, peer in enumerate((core_peer, x_peer, y_peer)):
        norm_send[stage] = part
        copy = pltpu.make_async_remote_copy(src_ref=norm_send.at[stage], dst_ref=norm_recv.at[stage], send_sem=norm_ssem.at[stage], recv_sem=norm_rsem.at[stage], device_id=(peer,), device_id_type=MESH_ID)
        copy.start()
        copy.wait()
        part = part + norm_recv[stage]
    norm_send[Z_PEERS] = part
    norm_recv[Z_PEERS + z_pos] = part
    z_copies = []
    for k in range(Z_PEERS):
        z_copies.append(pltpu.make_async_remote_copy(src_ref=norm_send.at[Z_PEERS], dst_ref=norm_recv.at[Z_PEERS + z_pos], send_sem=norm_ssem.at[Z_PEERS + k], recv_sem=norm_rsem.at[Z_PEERS + z_pos], device_id=(z_peers[k],), device_id_type=MESH_ID))
        z_copies[-1].start()
    for k in range(Z_PEERS):
        pltpu.make_async_remote_copy(src_ref=norm_send.at[Z_PEERS], dst_ref=norm_recv.at[Z_PEERS + z_others[k]], send_sem=norm_ssem.at[Z_PEERS + k], recv_sem=norm_rsem.at[Z_PEERS + z_others[k]], device_id=(z_peers[k],), device_id_type=MESH_ID).wait_recv()
    for k in range(Z_PEERS):
        z_copies[k].wait_send()
    sq_all = ((norm_recv[Z_PEERS] + norm_recv[Z_SIZE]) + norm_recv[5]) + norm_recv[6]
    norm_val = jnp.sqrt(sq_all)
    norm_ref[...] = norm_val
    lr_val = lr_ref[0, 0]
    scale = jnp.minimum(1.0, clip_ref[0, 0] / (norm_val + NORM_EPS))[0:1, :]

    def adam(g_val, p_val, m_val, v_val, s_val):
        scaled = s_val * (g_val * inv_dp)
        mom_new = BETA_ONE * m_val + (1.0 - BETA_ONE) * scaled
        var_new = BETA_TWO * v_val + (1.0 - BETA_TWO) * scaled * scaled
        return p_val - lr_val * (mom_new / BIAS_ONE) / (jnp.sqrt(var_new / BIAS_TWO) + ADAM_EPS), mom_new, var_new

    for base, (g_ref, p_ref, m_ref, v_ref, pn, mn, vn) in ((0, (g1, p1, m1, v1, p1n, m1n, v1n)), (W1_ROWS, (g3, p3, m3, v3, p3n, m3n, v3n))):
        for j in range(g_ref.shape[1] // LANES):
            cols = slice(j * LANES, (j + 1) * LANES)
            p_new, m_new, v_new = adam(g_ref[:, cols], p_ref[:, cols], m_ref[:, cols], v_ref[:, cols], scale)
            pn[:, cols] = p_new
            mn[:, cols] = m_new
            vn[:, cols] = v_new
            wide_p[base + OWN_ROWS * j:base + OWN_ROWS * (j + 1), :] = p_new
    wide_p[W1_ROWS + W3_ROWS:, :] = jnp.zeros((PACK_ROWS - W1_ROWS - W3_ROWS, LANES), jnp.float32)
    own_p[...] = wide_p[...].astype(jnp.bfloat16)
    scale_one = scale[0:1, 0:1]
    for base, (g_ref, p_ref, m_ref, v_ref, pn, mn, vn) in ((0, (g2, p2, m2, v2, p2n, m2n, v2n)), (TALL_ROWS, (g4, p4, m4, v4, p4n, m4n, v4n))):
        for r in range(g_ref.shape[0] // 16):
            rows = slice(r * 16, (r + 1) * 16)
            p_new, m_new, v_new = adam(g_ref[rows, :], p_ref[rows, :], m_ref[rows, :], v_ref[rows, :], scale_one)
            pn[rows, :] = p_new
            mn[rows, :] = m_new
            vn[rows, :] = v_new
            own_q[base + 16 * r:base + 16 * (r + 1), :] = p_new.astype(jnp.bfloat16)

    loc_p = pltpu.make_async_copy(own_p, all_p.at[me], local_sem.at[0])
    loc_q = pltpu.make_async_copy(own_q, all_q.at[me], local_sem.at[1])
    loc_p.start()
    loc_q.start()

    pending = []

    def send(buf, own, ssem, rsem, kind, slot, origin, peer, first):
        src = own if first else buf.at[origin]
        copy = pltpu.make_async_remote_copy(src_ref=src, dst_ref=buf.at[origin], send_sem=ssem.at[kind, slot], recv_sem=rsem.at[origin], device_id=(peer,), device_id_type=MESH_ID)
        copy.start()
        pending.append(copy)

    def arrive(buf, own, ssem, rsem, origin):
        pltpu.make_async_remote_copy(src_ref=own, dst_ref=buf.at[origin], send_sem=ssem.at[0, 0], recv_sem=rsem.at[origin], device_id=(core_peer,), device_id_type=MESH_ID).wait_recv()

    sets = ((all_p, own_p, send_p, recv_p, y_peer, x_peer, True), (all_q, own_q, send_q, recv_q, x_peer, y_peer, False))

    def origin_of(y_first, dz, da, db, dc=0):
        zo = (z_pos + dz) % Z_SIZE
        yo, xo = (da, db) if y_first else (db, da)
        return device_of((core + dc) % PAIR, (x_pos + xo) % PAIR, (y_pos + yo) % PAIR, zo)

    for buf, own, ssem, rsem, peer_a, peer_b, y_first in sets:
        send(buf, own, ssem, rsem, Z_PEERS, 0, me, peer_a, True)
        send(buf, own, ssem, rsem, Z_SIZE, 0, me, peer_b, True)
        for k in range(Z_PEERS):
            send(buf, own, ssem, rsem, k, 0, me, z_peers[k], True)
        send(buf, own, ssem, rsem, 5, 0, me, core_peer, True)
    steps = [(0, 1, 0)]
    for dz in (1, Z_PEERS, PAIR):
        steps += [(dz, 0, 0)]
    for dz in (1, Z_PEERS, PAIR):
        steps += [(dz, 1, 0)]
    for dz, da, _ in steps:
        for buf, own, ssem, rsem, peer_a, peer_b, y_first in sets:
            origin = origin_of(y_first, dz, da, 0)
            arrive(buf, own, ssem, rsem, origin)
            slot = dz * PAIR + da
            if da == 0:
                send(buf, own, ssem, rsem, Z_PEERS, dz, origin, peer_a, False)
            send(buf, own, ssem, rsem, Z_SIZE, slot, origin, peer_b, False)
            send(buf, own, ssem, rsem, 5, slot, origin, core_peer, False)
    for dz, da in [(0, 0), (0, 1), (1, 0), (Z_PEERS, 0), (PAIR, 0), (1, 1), (Z_PEERS, 1), (PAIR, 1)]:
        for buf, own, ssem, rsem, peer_a, peer_b, y_first in sets:
            origin = origin_of(y_first, dz, da, 1)
            arrive(buf, own, ssem, rsem, origin)
            send(buf, own, ssem, rsem, 5, 8 + dz * PAIR + da, origin, core_peer, False)
    for dz in range(Z_SIZE):
        for da in range(PAIR):
            for db in range(PAIR):
                for buf, own, ssem, rsem, peer_a, peer_b, y_first in sets:
                    arrive(buf, own, ssem, rsem, origin_of(y_first, dz, da, db, 1))
    for copy in pending:
        copy.wait_send()
    loc_p.wait()
    loc_q.wait()


def update_call(grads, masters, moms, variances, learn_rate, clip_max):
    f32 = jnp.float32
    bf16 = jnp.bfloat16
    vmem = pl.BlockSpec(memory_space=pltpu.VMEM)
    smem = pl.BlockSpec(memory_space=pltpu.SMEM)
    hbm = pl.BlockSpec(memory_space=pl.ANY)
    shapes = [jax.ShapeDtypeStruct(a.shape, f32) for a in masters]
    out_shape = [jax.ShapeDtypeStruct((DP_SIZE, PACK_ROWS, LANES), bf16), jax.ShapeDtypeStruct((DP_SIZE, STACK_ROWS, MODEL_DIM), bf16)] + shapes * Z_PEERS + [jax.ShapeDtypeStruct((8, LANES), f32)]
    return pl.pallas_call(
        update_kernel,
        out_shape=out_shape,
        in_specs=[vmem] * 16 + [smem] * PAIR,
        out_specs=[hbm, hbm] + [vmem] * 13,
        scratch_shapes=[
            pltpu.VMEM((PACK_ROWS, LANES), f32),
            pltpu.VMEM((PACK_ROWS, LANES), bf16),
            pltpu.VMEM((STACK_ROWS, MODEL_DIM), bf16),
            pltpu.VMEM((Z_SIZE, 8, LANES), f32),
            pltpu.VMEM((7, 8, LANES), f32),
            pltpu.SemaphoreType.DMA((6,)),
            pltpu.SemaphoreType.DMA((7,)),
            pltpu.SemaphoreType.DMA((6, 16)),
            pltpu.SemaphoreType.DMA((DP_SIZE,)),
            pltpu.SemaphoreType.DMA((6, 16)),
            pltpu.SemaphoreType.DMA((DP_SIZE,)),
            pltpu.SemaphoreType.DMA((PAIR,)),
        ],
        compiler_params=pltpu.CompilerParams(collective_id=0, has_side_effects=True, vmem_limit_bytes=40 * 1024 * 1024),
        name='adam_gather',
    )(*grads, *masters, *moms, *variances, learn_rate.reshape(1, 1), clip_max.reshape(1, 1))


def scatter_kernel(z_hbm, dh_hbm, dht_hbm, xt_hbm, w2_hbm, out1, out2,
                   dh, dht, xt, zbuf, w2c, a_even, a_odd, d_even, d_odd, acc1, acc2,
                   ra0, ra1, ra2, ra3, rb0, rb1, rb2, rb3, s1a, s2a, s3a, s1b, s2b, s3b, own2, qbuf,
                   in_sem, zsem, wsem, sa_send, sa_recv, sb_send, sb_recv, za_send, za_recv, zb_send, zb_recv, ga_send, ga_recv, fix_send, fix_recv):
    f32 = jnp.float32
    me = lax.axis_index('dp')
    core = me % PAIR
    x_pos = (me // PAIR) % PAIR
    y_pos = (me // Z_SIZE) % PAIR
    z_pos = me // 8
    core_peer = device_of(1 - core, x_pos, y_pos, z_pos)
    x_peer = device_of(core, 1 - x_pos, y_pos, z_pos)
    y_peer = device_of(core, x_pos, 1 - y_pos, z_pos)
    diag_peer = device_of(1 - core, 1 - x_pos, y_pos, z_pos)
    z_others = [(z_pos + k) % Z_SIZE for k in (1, PAIR, Z_PEERS)]
    z_peers = [device_of(core, x_pos, y_pos, zo) for zo in z_others]

    big = [pltpu.make_async_copy(src, dst, in_sem.at[i]) for i, (src, dst) in enumerate(((dh_hbm, dh), (dht_hbm, dht), (xt_hbm, xt)))]

    def chunk_copies(chunk):
        slot = chunk % PAIR
        zt = chunk % Z_SIZE
        k = chunk // Z_SIZE
        copies = []
        for b in range(Z_SIZE):
            off = pl.multiple_of(384 * (Z_SIZE * zt + b) + LANES * k, LANES)
            copies.append(pltpu.make_async_copy(z_hbm.at[:, pl.ds(off, LANES)], zbuf.at[slot, b], zsem.at[slot, b]))
            copies.append(pltpu.make_async_copy(w2_hbm.at[pl.ds(off, LANES), :], w2c.at[slot, pl.ds(b * LANES, LANES), :], wsem.at[slot, b]))
        return copies

    big[0].start()
    for copy in chunk_copies(0):
        copy.start()
    big[1].start()
    big[PAIR].start()
    qbuf[...] = jnp.zeros(qbuf.shape, f32)

    barrier = pltpu.get_barrier_semaphore()
    for peer in [core_peer, x_peer, y_peer, diag_peer] + z_peers:
        pl.semaphore_signal(barrier, inc=1, device_id=(peer,), device_id_type=MESH_ID)
    pl.semaphore_wait(barrier, 7)
    for copy in big:
        copy.wait()

    def remote(src, dst, ssem, rsem, peer):
        return pltpu.make_async_remote_copy(src_ref=src, dst_ref=dst, send_sem=ssem, recv_sem=rsem, device_id=(peer,), device_id_type=MESH_ID)

    def pair0(chunk):
        slot = chunk % PAIR
        return (remote(acc1.at[slot, 1 - core], ra0.at[slot], sa_send.at[0], sa_recv.at[0, slot], core_peer),
                remote(acc2.at[slot, :, :, 1 - core], rb0.at[slot], sb_send.at[0], sb_recv.at[0, slot], core_peer))

    def pair1(chunk):
        slot = chunk % PAIR
        return (remote(s1a.at[:, :, 1 - y_pos], ra1.at[slot], sa_send.at[1], sa_recv.at[1, slot], y_peer),
                remote(s1b.at[:, 1 - x_pos], rb1.at[slot], sb_send.at[1], sb_recv.at[1, slot], x_peer))

    def pair2(chunk):
        slot = chunk % PAIR
        return (remote(s2a.at[1 - x_pos], ra2.at[slot], sa_send.at[PAIR], sa_recv.at[PAIR, slot], x_peer),
                remote(s2b.at[1 - y_pos], rb2.at[slot], sb_send.at[PAIR], sb_recv.at[PAIR, slot], y_peer))

    def z_send_a(chunk):
        slot = chunk % PAIR
        return [remote(s3a.at[z_others[k]], ra3.at[slot, z_pos], za_send.at[k], za_recv.at[slot, z_pos], z_peers[k]) for k in range(Z_PEERS)]

    def z_recv_a(chunk):
        slot = chunk % PAIR
        return [remote(s3a.at[z_others[k]], ra3.at[slot, z_others[k]], za_send.at[k], za_recv.at[slot, z_others[k]], z_peers[k]) for k in range(Z_PEERS)]

    def z_send_b(chunk):
        zt = chunk % Z_SIZE
        return remote(s3b, rb3.at[chunk // Z_SIZE, z_pos], zb_send.at[0], zb_recv.at[chunk // Z_SIZE, z_pos], device_of(core, x_pos, y_pos, zt))

    def z_recv_b(chunk):
        return [remote(s3b, rb3.at[chunk // Z_SIZE, z_others[k]], zb_send.at[0], zb_recv.at[chunk // Z_SIZE, z_others[k]], z_peers[k]) for k in range(Z_PEERS)]

    lane_me = core * PAIR + x_pos
    group = ((1 - core, x_pos, core_peer), (core, 1 - x_pos, x_peer), (1 - core, 1 - x_pos, diag_peer))

    def g_send(chunk):
        slot = chunk % PAIR
        return [remote(qbuf.at[gx * PAIR + gc], out1.at[lane_me, chunk], ga_send.at[i], ga_recv.at[i, slot], peer) for i, (gc, gx, peer) in enumerate(group)]

    def g_recv(chunk):
        slot = chunk % PAIR
        return [remote(qbuf.at[gx * PAIR + gc], out1.at[gc * PAIR + gx, chunk], ga_send.at[i], ga_recv.at[i, slot], peer) for i, (gc, gx, peer) in enumerate(group)]

    def within(t, lead):
        return jnp.logical_and(t >= lead, t < lead + CHUNKS)

    def elementwise(slot, r, a_buf, d_buf):
        rows = pl.ds(pl.multiple_of(r * TILE_R, TILE_R), TILE_R)
        back = lax.dot_general(dh[rows, :], w2c[slot], (((1,), (1,)), ((), ())), preferred_element_type=f32).astype(jnp.bfloat16)
        for b in range(Z_SIZE):
            cols = slice(b * LANES, (b + 1) * LANES)
            wide = zbuf[slot, b, rows, :].astype(f32)
            cdf = 0.5 * (1.0 + lax.erf(wide * INV_SQRT2))
            a_buf[:, cols] = (wide * cdf).astype(jnp.bfloat16)
            slope = cdf + wide * INV_SQRT2PI * jnp.exp(-0.5 * wide * wide)
            d_buf[:, cols] = (back[:, cols].astype(f32) * slope).astype(jnp.bfloat16)

    def accumulate(slot, r, a_buf, d_buf, first):
        rows = pl.ds(pl.multiple_of(r * TILE_R, TILE_R), TILE_R)
        part1 = jnp.dot(xt[:, rows], d_buf[...], preferred_element_type=f32)
        part2 = jnp.dot(dht[:, rows], a_buf[...], preferred_element_type=f32)
        for b in range(Z_SIZE):
            c1, x1 = b // PAIR, b % PAIR
            val1 = part1[:, b * LANES:(b + 1) * LANES].reshape(Z_SIZE, PAIR, GROUP_ROWS, LANES)
            val2 = part2[:, b * LANES:(b + 1) * LANES].reshape(PAIR, HALF_ROWS, LANES)
            if first:
                acc1[slot, c1, x1] = val1
                acc2[slot, b // PAIR, b % PAIR] = val2
            else:
                acc1[slot, c1, x1] = acc1[slot, c1, x1] + val1
                acc2[slot, b // PAIR, b % PAIR] = acc2[slot, b // PAIR, b % PAIR] + val2

    n_tiles = ROWS_DEV // TILE_R

    def compute(chunk):
        slot = chunk % PAIR
        for copy in chunk_copies(chunk):
            copy.wait()

        @pl.when(chunk + 1 < CHUNKS)
        def _():
            for copy in chunk_copies(chunk + 1):
                copy.start()

        elementwise(slot, 0, a_even, d_even)
        elementwise(slot, 1, a_odd, d_odd)
        accumulate(slot, 0, a_even, d_even, True)

        def body(i, carry):
            elementwise(slot, PAIR * i, a_even, d_even)
            accumulate(slot, PAIR * i - 1, a_odd, d_odd, False)
            elementwise(slot, PAIR * i + 1, a_odd, d_odd)
            accumulate(slot, PAIR * i, a_even, d_even, False)
            return carry

        lax.fori_loop(1, n_tiles // PAIR, body, 0)
        accumulate(slot, n_tiles - 1, a_odd, d_odd, False)

    def step(t, carry):
        @pl.when(within(t, 6))
        def _():
            for copy in g_send(t - 6):
                copy.wait_send()
            for copy in g_recv(t - 6):
                copy.wait_recv()

        @pl.when(within(t, 5))
        def _():
            chunk = t - 5
            slot = chunk % PAIR
            zt = chunk % Z_SIZE
            for copy in z_send_a(chunk):
                copy.wait_send()
            for copy in z_recv_a(chunk):
                copy.wait_recv()
            full = s3a[z_pos] + ra3[slot, z_others[0]] + ra3[slot, z_others[1]] + ra3[slot, z_others[PAIR]]
            for o in range(Z_SIZE):
                qbuf[o, 0:OWN_ROWS, :] = full[OWN_ROWS * o:OWN_ROWS * (o + 1), :]
            out1[lane_me, chunk] = qbuf[x_pos * PAIR + core]

            @pl.when(z_pos == zt)
            def _():
                for copy in z_recv_b(chunk):
                    copy.wait_recv()
                k = chunk // Z_SIZE
                own2[k] = s3b[...] + rb3[k, z_others[0]] + rb3[k, z_others[1]] + rb3[k, z_others[PAIR]]

            @pl.when(z_pos != zt)
            def _():
                z_send_b(chunk).wait_send()

        @pl.when(within(t, Z_SIZE))
        def _():
            chunk = t - Z_SIZE
            slot = chunk % PAIR
            for copy in pair2(chunk):
                copy.wait()
            for z in range(Z_SIZE):
                s3a[z] = s2a[x_pos, z] + ra2[slot, z]
            s3b[...] = s2b[y_pos] + rb2[slot]

        @pl.when(within(t, Z_PEERS))
        def _():
            chunk = t - Z_PEERS
            slot = chunk % PAIR
            for copy in pair1(chunk):
                copy.wait()
            for x in range(PAIR):
                for z in range(Z_SIZE):
                    s2a[x, z] = s1a[x, z, y_pos] + ra1[slot, x, z]
            for y in range(PAIR):
                s2b[y] = s1b[y, x_pos] + rb1[slot, y]

        @pl.when(within(t, PAIR))
        def _():
            chunk = t - PAIR
            slot = chunk % PAIR
            for copy in pair0(chunk):
                copy.wait()
            for x in range(PAIR):
                s1a[x] = acc1[slot, core, x] + ra0[slot, x]
            for y in range(PAIR):
                for x in range(PAIR):
                    s1b[y, x] = acc2[slot, y, x, core] + rb0[slot, y, x]

        @pl.when(within(t, 1))
        def _():
            for copy in pair0(t - 1):
                copy.start()

        @pl.when(within(t, PAIR))
        def _():
            for copy in pair1(t - PAIR):
                copy.start()

        @pl.when(within(t, Z_PEERS))
        def _():
            for copy in pair2(t - Z_PEERS):
                copy.start()

        @pl.when(within(t, Z_SIZE))
        def _():
            chunk = t - Z_SIZE
            for copy in z_send_a(chunk):
                copy.start()

            @pl.when(z_pos != chunk % Z_SIZE)
            def _():
                z_send_b(chunk).start()

        @pl.when(within(t, 5))
        def _():
            for copy in g_send(t - 5):
                copy.start()

        @pl.when(t < CHUNKS)
        def _():
            compute(t)

        return carry

    lax.fori_loop(0, CHUNKS + 6, step, 0)

    fixes = [remote(own2.at[1 - core + i], out2.at[i, core], fix_send.at[i], fix_recv.at[i], core_peer) for i in range(PAIR)]
    for copy in fixes:
        copy.start()
    for i in range(PAIR):
        out2[i, core] = own2[core + i]
    for i in range(PAIR):
        remote(own2.at[1 - core + i], out2.at[i, 1 - core], fix_send.at[i], fix_recv.at[i], core_peer).wait()


def scatter_call(z_one, dh_two, dh_two_t, x_t, w_two):
    f32 = jnp.float32
    bf16 = jnp.bfloat16
    hbm = pl.BlockSpec(memory_space=pl.ANY)
    vmem = pl.BlockSpec(memory_space=pltpu.VMEM)
    dma = pltpu.SemaphoreType.DMA
    buf = pltpu.VMEM
    return pl.pallas_call(
        scatter_kernel,
        out_shape=[jax.ShapeDtypeStruct((Z_SIZE, CHUNKS, PAD_ROWS, LANES), f32), jax.ShapeDtypeStruct((PAIR, PAIR, HALF_ROWS, LANES), f32)],
        in_specs=[hbm] * 5,
        out_specs=[vmem, vmem],
        scratch_shapes=[
            buf((ROWS_DEV, MODEL_DIM), bf16), buf((MODEL_DIM, ROWS_DEV), bf16), buf((MODEL_DIM, ROWS_DEV), bf16),
            buf((PAIR, Z_SIZE, ROWS_DEV, LANES), bf16), buf((PAIR, CHUNK_W, MODEL_DIM), bf16),
            buf((TILE_R, CHUNK_W), bf16), buf((TILE_R, CHUNK_W), bf16), buf((TILE_R, CHUNK_W), bf16), buf((TILE_R, CHUNK_W), bf16),
            buf((PAIR, PAIR, PAIR, Z_SIZE, PAIR, GROUP_ROWS, LANES), f32), buf((PAIR, PAIR, PAIR, PAIR, HALF_ROWS, LANES), f32),
            buf((PAIR, PAIR, Z_SIZE, PAIR, GROUP_ROWS, LANES), f32), buf((PAIR, PAIR, Z_SIZE, GROUP_ROWS, LANES), f32), buf((PAIR, Z_SIZE, GROUP_ROWS, LANES), f32), buf((PAIR, Z_SIZE, GROUP_ROWS, LANES), f32),
            buf((PAIR, PAIR, PAIR, HALF_ROWS, LANES), f32), buf((PAIR, PAIR, HALF_ROWS, LANES), f32), buf((PAIR, HALF_ROWS, LANES), f32), buf((Z_PEERS, Z_SIZE, HALF_ROWS, LANES), f32),
            buf((PAIR, Z_SIZE, PAIR, GROUP_ROWS, LANES), f32), buf((PAIR, Z_SIZE, GROUP_ROWS, LANES), f32), buf((Z_SIZE, GROUP_ROWS, LANES), f32),
            buf((PAIR, PAIR, HALF_ROWS, LANES), f32), buf((PAIR, HALF_ROWS, LANES), f32), buf((HALF_ROWS, LANES), f32),
            buf((Z_PEERS, HALF_ROWS, LANES), f32), buf((Z_SIZE, PAD_ROWS, LANES), f32),
            dma((Z_PEERS,)), dma((PAIR, Z_SIZE)), dma((PAIR, Z_SIZE)),
            dma((Z_PEERS,)), dma((Z_PEERS, PAIR)), dma((Z_PEERS,)), dma((Z_PEERS, PAIR)),
            dma((Z_PEERS,)), dma((PAIR, Z_SIZE)), dma((1,)), dma((Z_PEERS, Z_SIZE)),
            dma((Z_PEERS,)), dma((Z_PEERS, PAIR)), dma((PAIR,)), dma((PAIR,)),
        ],
        compiler_params=pltpu.CompilerParams(collective_id=1, has_side_effects=True, vmem_limit_bytes=60 * 1024 * 1024),
        cost_estimate=pl.CostEstimate(flops=100_000_000_000, bytes_accessed=80_000_000, transcendentals=50_000_000),
        name='grad_scatter',
    )(z_one, dh_two, dh_two_t, x_t, w_two)


def forward_kernel(x_ref, dy_ref, w1, w2, w3, w4, z_out, dh_out, dht_out, xt_out, g3_out, g4t_out,
                   h_acc, a_even, a_odd, h_t, dy_t):
    f32 = jnp.float32
    bf16 = jnp.bfloat16

    @pl.when(pl.program_id(0) == 0)
    def _():
        g3_out[...] = jnp.zeros(g3_out.shape, f32)
        g4t_out[...] = jnp.zeros(g4t_out.shape, f32)

    def hidden(c, a_buf):
        cols = pl.ds(pl.multiple_of(c * CHUNK_W, CHUNK_W), CHUNK_W)
        z_val = jnp.dot(x_ref[...], w1[:, cols], preferred_element_type=f32).astype(bf16)
        z_out[:, cols] = z_val
        a_buf[...] = gelu_value(z_val).astype(bf16)

    def project(c, a_buf, first):
        rows = pl.ds(pl.multiple_of(c * CHUNK_W, CHUNK_W), CHUNK_W)
        part = jnp.dot(a_buf[...], w2[rows, :], preferred_element_type=f32)
        if first:
            h_acc[...] = part
        else:
            h_acc[...] = h_acc[...] + part

    xt_out[...] = x_ref[...].T
    dy_t[...] = dy_ref[...].T
    hidden(0, a_even)
    hidden(1, a_odd)
    project(0, a_even, True)

    def body(i, carry):
        hidden(PAIR * i, a_even)
        project(PAIR * i - 1, a_odd, False)
        hidden(PAIR * i + 1, a_odd)
        project(PAIR * i, a_even, False)
        return carry

    lax.fori_loop(1, CHUNKS // PAIR, body, 0)
    project(CHUNKS - 1, a_odd, False)
    h_two = h_acc[...].astype(bf16)
    h_t[...] = h_two.T
    dh_sum = None
    for j in range(w3.shape[1] // CHUNK_W):
        cols = slice(j * CHUNK_W, (j + 1) * CHUNK_W)
        z_three = jnp.dot(h_two, w3[:, cols], preferred_element_type=f32).astype(bf16)
        wide = z_three.astype(f32)
        cdf = 0.5 * (1.0 + lax.erf(wide * INV_SQRT2))
        a_three = (wide * cdf).astype(bf16)
        slope = cdf + wide * INV_SQRT2PI * jnp.exp(-0.5 * wide * wide)
        da_three = lax.dot_general(dy_ref[...], w4[cols, :], (((1,), (1,)), ((), ())), preferred_element_type=f32).astype(bf16)
        dz_three = (da_three.astype(f32) * slope).astype(bf16)
        g4t_out[:, cols] = g4t_out[:, cols] + jnp.dot(dy_t[...], a_three, preferred_element_type=f32)
        g3_out[:, cols] = g3_out[:, cols] + jnp.dot(h_t[...], dz_three, preferred_element_type=f32)
        part = lax.dot_general(dz_three, w3[:, cols], (((1,), (1,)), ((), ())), preferred_element_type=f32)
        dh_sum = part if dh_sum is None else dh_sum + part
    dh_two = dh_sum.astype(bf16)
    dh_out[...] = dh_two
    dht_out[...] = dh_two.T


def forward_call(x_rows, dy_rows, w_one, w_two, w_three, w_four):
    f32 = jnp.float32
    bf16 = jnp.bfloat16
    buf = pltpu.VMEM
    rows_in = pl.BlockSpec((TILE_R, MODEL_DIM), lambda i: (i, 0))
    cols_out = pl.BlockSpec((MODEL_DIM, TILE_R), lambda i: (0, i))
    whole = lambda a: pl.BlockSpec(a.shape, lambda i: (0, 0), pipeline_mode=pl.Buffered(1))
    small = jax.ShapeDtypeStruct((MODEL_DIM, FF_DIM), f32)
    tall = jax.ShapeDtypeStruct((ROWS_DEV, MODEL_DIM), bf16)
    flat = jax.ShapeDtypeStruct((MODEL_DIM, ROWS_DEV), bf16)
    return pl.pallas_call(
        forward_kernel,
        grid=(ROWS_DEV // TILE_R,),
        out_shape=[jax.ShapeDtypeStruct((ROWS_DEV, WIDE_DIM), bf16), tall, flat, flat, small, small],
        in_specs=[rows_in, rows_in] + [whole(a) for a in (w_one, w_two, w_three, w_four)],
        out_specs=[pl.BlockSpec((TILE_R, WIDE_DIM), lambda i: (i, 0)), rows_in, cols_out, cols_out, whole(small), whole(small)],
        scratch_shapes=[buf((TILE_R, MODEL_DIM), f32), buf((TILE_R, CHUNK_W), bf16), buf((TILE_R, CHUNK_W), bf16), buf((MODEL_DIM, TILE_R), bf16), buf((MODEL_DIM, TILE_R), bf16)],
        compiler_params=pltpu.CompilerParams(vmem_limit_bytes=60 * 1024 * 1024),
        cost_estimate=pl.CostEstimate(flops=100_000_000_000, bytes_accessed=100_000_000, transcendentals=50_000_000),
        name='forward_chain',
    )(x_rows, dy_rows, w_one, w_two, w_three, w_four)


def unpack_kernel(p_ref, q_ref, w1_out, w2_out, w3_out, w4_out, wide, lane_buf):
    owners = p_ref.shape[0]
    for o in range(owners):
        wide[o] = p_ref[o].astype(jnp.float32)
        w2_out[o * TALL_ROWS:(o + 1) * TALL_ROWS, :] = q_ref[o, :TALL_ROWS, :]
        w4_out[o * SHORT_ROWS:(o + 1) * SHORT_ROWS, :] = q_ref[o, TALL_ROWS:, :]
    for w_out, base in ((w1_out, 0), (w3_out, W1_ROWS)):
        for j in range(w_out.shape[1] // LANES):
            for o in range(owners):
                lane_buf[j % PAIR, o * OWN_ROWS:(o + 1) * OWN_ROWS, :] = wide[o, base + j * OWN_ROWS:base + (j + 1) * OWN_ROWS, :]
            w_out[:, j * LANES:(j + 1) * LANES] = lane_buf[j % PAIR].astype(jnp.bfloat16)


def unpack_call(all_p, all_q):
    f32 = jnp.float32
    bf16 = jnp.bfloat16
    owners = 8
    shapes = ((MODEL_DIM, WIDE_DIM), (WIDE_DIM, MODEL_DIM), (MODEL_DIM, FF_DIM), (FF_DIM, MODEL_DIM))
    steps = DP_SIZE // owners
    return pl.pallas_call(
        unpack_kernel,
        grid=(steps,),
        out_shape=[jax.ShapeDtypeStruct(s, bf16) for s in shapes],
        in_specs=[pl.BlockSpec((owners, PACK_ROWS, LANES), lambda i: (i, 0, 0)), pl.BlockSpec((owners, STACK_ROWS, MODEL_DIM), lambda i: (i, 0, 0))],
        out_specs=[pl.BlockSpec((s[0] // steps, s[1]), lambda i: (i, 0)) for s in shapes],
        scratch_shapes=[pltpu.VMEM((owners, PACK_ROWS, LANES), f32), pltpu.VMEM((PAIR, owners * OWN_ROWS, LANES), f32)],
        compiler_params=pltpu.CompilerParams(vmem_limit_bytes=SHORT_ROWS * 1024 * 1024),
        name='unpack_weights',
    )(all_p, all_q)


def solution(mesh):
    row_spec = P('dp', None)
    rep_spec = P()

    def per_device(x_rows, dy_rows, w_one, w_two, w_three, w_four, master_one, master_two, master_three, master_four, m_one, m_two, m_three, m_four, v_one, v_two, v_three, v_four, learn_rate, clip_max):
        z_one, dh_two, dh_two_t, x_t, g_three, g_four_t = forward_call(x_rows, dy_rows, w_one, w_two, w_three, w_four)
        s_four = lax.psum_scatter(g_four_t.T, 'dp', scatter_dimension=0, tiled=True)
        s_three = lax.psum_scatter(g_three.reshape(-1, LANES), 'dp', scatter_dimension=0, tiled=True).reshape(OWN_ROWS, FF_DIM)
        sum_one, sum_two = scatter_call(z_one, dh_two, dh_two_t, x_t, w_two)
        s_one = sum_one.reshape(Z_SIZE, Z_PEERS, Z_SIZE, PAD_ROWS, LANES)[:, :, :, :OWN_ROWS].transpose(Z_PEERS, PAIR, 0, 1, Z_SIZE).reshape(OWN_ROWS, WIDE_DIM)
        flat_two = sum_two.transpose(1, PAIR, 0, Z_PEERS).reshape(MODEL_DIM, 256)
        s_two = lax.dynamic_slice_in_dim(flat_two, 64 * (lax.axis_index('dp') % PAIR), TALL_ROWS, axis=1).T
        outs = update_call((s_one, s_two, s_three, s_four), (master_one, master_two, master_three, master_four), (m_one, m_two, m_three, m_four), (v_one, v_two, v_three, v_four), learn_rate, clip_max)
        w1n, w2n, w3n, w4n = unpack_call(outs[0], outs[1])
        return (w1n, w2n, w3n, w4n) + tuple(outs[PAIR:14]) + (outs[14][0, 0],)

    in_specs = (row_spec, row_spec) + (rep_spec,) * Z_SIZE + (row_spec,) * 12 + (rep_spec, rep_spec)
    out_specs = (rep_spec,) * Z_SIZE + (row_spec,) * 12 + (rep_spec,)
    return jax.shard_map(per_device, mesh=mesh, in_specs=in_specs, out_specs=out_specs, check_vma=False)
```

```python
import jax
import jax.numpy as jnp
from jax import lax
from jax.experimental import pallas as pl
from jax.experimental.pallas import tpu as pltpu
from jax.sharding import PartitionSpec as P

ADAM_STEP = 10
BETA_ONE = 0.9
BETA_TWO = 0.95
ADAM_EPS = 1e-8
NORM_EPS = 1e-6
BIAS_ONE = 1.0 - BETA_ONE ** ADAM_STEP
BIAS_TWO = 1.0 - BETA_TWO ** ADAM_STEP
INV_SQRT2 = 0.7071067811865476
INV_SQRT2PI = 0.3989422804014327
DP_SIZE = 32
MESH_ID = pl.DeviceIdType.MESH
W1_ROWS = 48 * 18
W3_ROWS = 12 * 18
PACK_ROWS = 1088
CHUNKS = 12
CHUNK_W = 512
ROWS_DEV = 4096
TILE_R = 512
LANES = 128
MODEL_DIM = 576
GROUP_ROWS = 72
HALF_ROWS = 288
OWN_ROWS = 18
Z_SIZE = 4
PAIR = 2
ACC_SLOTS = 3
Z_PEERS = 3
PAD_ROWS = 24
WIDE_DIM = 6144
FF_DIM = 1536
STACK_ROWS = 240
TALL_ROWS = 192
SHORT_ROWS = 48


def gelu_value(pre_act):
    pre_wide = pre_act.astype(jnp.float32)
    return 0.5 * pre_wide * (1.0 + lax.erf(pre_wide * INV_SQRT2))


def device_of(core, x_pos, y_pos, z_pos):
    return ((z_pos * PAIR + y_pos) * PAIR + x_pos) * PAIR + core


def adam_new(g_val, p_val, m_val, v_val, s_val, lr_val):
    scaled = s_val * (g_val * (1.0 / DP_SIZE))
    mom_new = BETA_ONE * m_val + (1.0 - BETA_ONE) * scaled
    var_new = BETA_TWO * v_val + (1.0 - BETA_TWO) * scaled * scaled
    return p_val - lr_val * (mom_new / BIAS_ONE) / (jnp.sqrt(var_new / BIAS_TWO) + ADAM_EPS), mom_new, var_new


def update_kernel(*refs):
    sources, (lr_ref, clip_ref, all_p, all_q, norm_ref), locals_, rest = refs[:16], refs[16:21], refs[21:37], refs[37:]
    wide_p, own_p, own_q, norm_send, norm_recv, norm_ssem, norm_rsem, send_p, recv_p, send_q, recv_q, local_sem, load_sem = rest
    g1, g2, g3, g4, p1, p2, p3, p4, m1, m2, m3, m4, v1, v2, v3, v4 = locals_
    loads = [pltpu.make_async_copy(src, dst, load_sem.at[i]) for i, (src, dst) in enumerate(zip(sources, locals_))]
    for copy in loads:
        copy.start()
    me = lax.axis_index('dp')
    core = me % PAIR
    x_pos = (me // PAIR) % PAIR
    y_pos = (me // Z_SIZE) % PAIR
    z_pos = me // 8
    core_peer = device_of(1 - core, x_pos, y_pos, z_pos)
    x_peer = device_of(core, 1 - x_pos, y_pos, z_pos)
    y_peer = device_of(core, x_pos, 1 - y_pos, z_pos)
    z_others = [(z_pos + k) % Z_SIZE for k in (1, PAIR, Z_PEERS)]
    z_peers = [device_of(core, x_pos, y_pos, zo) for zo in z_others]

    barrier = pltpu.get_barrier_semaphore()
    for peer in [core_peer, x_peer, y_peer] + z_peers:
        pl.semaphore_signal(barrier, inc=1, device_id=(peer,), device_id_type=MESH_ID)
    pl.semaphore_wait(barrier, 6)

    for copy in loads:
        copy.wait()
    inv_dp = 1.0 / DP_SIZE
    total = jnp.zeros((1, LANES), jnp.float32)
    for g_ref in (g1, g3):
        for j in range(g_ref.shape[1] // LANES):
            g_val = g_ref[:, j * LANES:(j + 1) * LANES] * inv_dp
            total = total + jnp.sum(g_val * g_val, axis=0, keepdims=True)
    scal = jnp.sum(total)
    for g_ref in (g2, g4):
        g_val = g_ref[...] * inv_dp
        scal = scal + jnp.sum(g_val * g_val)
    part = jnp.full((8, LANES), scal, jnp.float32)
    for stage, peer in enumerate((core_peer, x_peer, y_peer)):
        norm_send[stage] = part
        copy = pltpu.make_async_remote_copy(src_ref=norm_send.at[stage], dst_ref=norm_recv.at[stage], send_sem=norm_ssem.at[stage], recv_sem=norm_rsem.at[stage], device_id=(peer,), device_id_type=MESH_ID)
        copy.start()
        copy.wait()
        part = part + norm_recv[stage]
    norm_send[Z_PEERS] = part
    norm_recv[Z_PEERS + z_pos] = part
    z_copies = []
    for k in range(Z_PEERS):
        z_copies.append(pltpu.make_async_remote_copy(src_ref=norm_send.at[Z_PEERS], dst_ref=norm_recv.at[Z_PEERS + z_pos], send_sem=norm_ssem.at[Z_PEERS + k], recv_sem=norm_rsem.at[Z_PEERS + z_pos], device_id=(z_peers[k],), device_id_type=MESH_ID))
        z_copies[-1].start()
    for k in range(Z_PEERS):
        pltpu.make_async_remote_copy(src_ref=norm_send.at[Z_PEERS], dst_ref=norm_recv.at[Z_PEERS + z_others[k]], send_sem=norm_ssem.at[Z_PEERS + k], recv_sem=norm_rsem.at[Z_PEERS + z_others[k]], device_id=(z_peers[k],), device_id_type=MESH_ID).wait_recv()
    for k in range(Z_PEERS):
        z_copies[k].wait_send()
    sq_all = ((norm_recv[Z_PEERS] + norm_recv[Z_SIZE]) + norm_recv[5]) + norm_recv[6]
    norm_val = jnp.sqrt(sq_all)
    norm_ref[...] = norm_val
    lr_val = lr_ref[0, 0]
    scale = jnp.minimum(1.0, clip_ref[0, 0] / (norm_val + NORM_EPS))[0:1, :]

    for base, (g_ref, p_ref, m_ref, v_ref) in ((0, (g1, p1, m1, v1)), (W1_ROWS, (g3, p3, m3, v3))):
        for j in range(g_ref.shape[1] // LANES):
            cols = slice(j * LANES, (j + 1) * LANES)
            p_new = adam_new(g_ref[:, cols], p_ref[:, cols], m_ref[:, cols], v_ref[:, cols], scale, lr_val)[0]
            wide_p[base + OWN_ROWS * j:base + OWN_ROWS * (j + 1), :] = p_new
    wide_p[W1_ROWS + W3_ROWS:, :] = jnp.zeros((PACK_ROWS - W1_ROWS - W3_ROWS, LANES), jnp.float32)
    own_p[...] = wide_p[...].astype(jnp.bfloat16)
    scale_one = scale[0:1, 0:1]
    for base, (g_ref, p_ref, m_ref, v_ref) in ((0, (g2, p2, m2, v2)), (TALL_ROWS, (g4, p4, m4, v4))):
        for r in range(g_ref.shape[0] // 16):
            rows = slice(r * 16, (r + 1) * 16)
            p_new = adam_new(g_ref[rows, :], p_ref[rows, :], m_ref[rows, :], v_ref[rows, :], scale_one, lr_val)[0]
            own_q[base + 16 * r:base + 16 * (r + 1), :] = p_new.astype(jnp.bfloat16)

    loc_p = pltpu.make_async_copy(own_p, all_p.at[me], local_sem.at[0])
    loc_q = pltpu.make_async_copy(own_q, all_q.at[me], local_sem.at[1])
    loc_p.start()
    loc_q.start()

    pending = []

    def send(buf, own, ssem, rsem, kind, slot, origin, peer, first):
        src = own if first else buf.at[origin]
        copy = pltpu.make_async_remote_copy(src_ref=src, dst_ref=buf.at[origin], send_sem=ssem.at[kind, slot], recv_sem=rsem.at[origin], device_id=(peer,), device_id_type=MESH_ID)
        copy.start()
        pending.append(copy)

    def arrive(buf, own, ssem, rsem, origin):
        pltpu.make_async_remote_copy(src_ref=own, dst_ref=buf.at[origin], send_sem=ssem.at[0, 0], recv_sem=rsem.at[origin], device_id=(core_peer,), device_id_type=MESH_ID).wait_recv()

    sets = ((all_p, own_p, send_p, recv_p, y_peer, x_peer, True), (all_q, own_q, send_q, recv_q, x_peer, y_peer, False))

    def origin_of(y_first, dz, da, db, dc=0):
        zo = (z_pos + dz) % Z_SIZE
        yo, xo = (da, db) if y_first else (db, da)
        return device_of((core + dc) % PAIR, (x_pos + xo) % PAIR, (y_pos + yo) % PAIR, zo)

    for buf, own, ssem, rsem, peer_a, peer_b, y_first in sets:
        send(buf, own, ssem, rsem, Z_PEERS, 0, me, peer_a, True)
        send(buf, own, ssem, rsem, Z_SIZE, 0, me, peer_b, True)
        for k in range(Z_PEERS):
            send(buf, own, ssem, rsem, k, 0, me, z_peers[k], True)
        send(buf, own, ssem, rsem, 5, 0, me, core_peer, True)
    steps = [(0, 1, 0)]
    for dz in (1, Z_PEERS, PAIR):
        steps += [(dz, 0, 0)]
    for dz in (1, Z_PEERS, PAIR):
        steps += [(dz, 1, 0)]
    for dz, da, _ in steps:
        for buf, own, ssem, rsem, peer_a, peer_b, y_first in sets:
            origin = origin_of(y_first, dz, da, 0)
            arrive(buf, own, ssem, rsem, origin)
            slot = dz * PAIR + da
            if da == 0:
                send(buf, own, ssem, rsem, Z_PEERS, dz, origin, peer_a, False)
            send(buf, own, ssem, rsem, Z_SIZE, slot, origin, peer_b, False)
            send(buf, own, ssem, rsem, 5, slot, origin, core_peer, False)
    for dz, da in [(0, 0), (0, 1), (1, 0), (Z_PEERS, 0), (PAIR, 0), (1, 1), (Z_PEERS, 1), (PAIR, 1)]:
        for buf, own, ssem, rsem, peer_a, peer_b, y_first in sets:
            origin = origin_of(y_first, dz, da, 1)
            arrive(buf, own, ssem, rsem, origin)
            send(buf, own, ssem, rsem, 5, 8 + dz * PAIR + da, origin, core_peer, False)
    for dz in range(Z_SIZE):
        for da in range(PAIR):
            for db in range(PAIR):
                for buf, own, ssem, rsem, peer_a, peer_b, y_first in sets:
                    arrive(buf, own, ssem, rsem, origin_of(y_first, dz, da, db, 1))
    for copy in pending:
        copy.wait_send()
    loc_p.wait()
    loc_q.wait()


def update_call(states, learn_rate, clip_max):
    f32 = jnp.float32
    bf16 = jnp.bfloat16
    dma = pltpu.SemaphoreType.DMA
    buf = pltpu.VMEM
    smem = pl.BlockSpec(memory_space=pltpu.SMEM)
    hbm = pl.BlockSpec(memory_space=pl.ANY)
    vmem = pl.BlockSpec(memory_space=pltpu.VMEM)
    kinds = 6
    return pl.pallas_call(
        update_kernel,
        out_shape=[jax.ShapeDtypeStruct((DP_SIZE, PACK_ROWS, LANES), bf16), jax.ShapeDtypeStruct((DP_SIZE, STACK_ROWS, MODEL_DIM), bf16), jax.ShapeDtypeStruct((8, LANES), f32)],
        in_specs=[hbm] * len(states) + [smem, smem],
        out_specs=[hbm, hbm, vmem],
        scratch_shapes=[buf(a.shape, f32) for a in states] + [
            buf((PACK_ROWS, LANES), f32), buf((PACK_ROWS, LANES), bf16), buf((STACK_ROWS, MODEL_DIM), bf16),
            buf((Z_SIZE, 8, LANES), f32), buf((7, 8, LANES), f32), dma((kinds,)), dma((7,)),
            dma((kinds, 16)), dma((DP_SIZE,)), dma((kinds, 16)), dma((DP_SIZE,)), dma((PAIR,)), dma((len(states),)),
        ],
        compiler_params=pltpu.CompilerParams(collective_id=0, has_side_effects=True, vmem_limit_bytes=60 * 1024 * 1024),
        name='adam_gather',
    )(*states, learn_rate.reshape(1, 1), clip_max.reshape(1, 1))


def scatter_kernel(z_hbm, dh_hbm, dht_hbm, xt_hbm, w2_hbm, out1, out2,
                   dh, dht, xt, zbuf, w2c, a_even, a_odd, d_even, d_odd, acc1, acc2,
                   ra0, ra1, ra2, ra3, rb0, rb1, rb2, rb3, s1a, s2a, s3a, s1b, s2b, s3b, own2, qbuf,
                   in_sem, zsem, wsem, sa_send, sa_recv, sb_send, sb_recv, za_send, za_recv, zb_send, zb_recv, ga_send, ga_recv, fix_send, fix_recv):
    f32 = jnp.float32
    me = lax.axis_index('dp')
    core = me % PAIR
    x_pos = (me // PAIR) % PAIR
    y_pos = (me // Z_SIZE) % PAIR
    z_pos = me // 8
    core_peer = device_of(1 - core, x_pos, y_pos, z_pos)
    x_peer = device_of(core, 1 - x_pos, y_pos, z_pos)
    y_peer = device_of(core, x_pos, 1 - y_pos, z_pos)
    diag_peer = device_of(1 - core, 1 - x_pos, y_pos, z_pos)
    z_others = [(z_pos + k) % Z_SIZE for k in (1, PAIR, Z_PEERS)]
    z_peers = [device_of(core, x_pos, y_pos, zo) for zo in z_others]

    big = [pltpu.make_async_copy(src, dst, in_sem.at[i]) for i, (src, dst) in enumerate(((dh_hbm, dh), (dht_hbm, dht), (xt_hbm, xt)))]

    def chunk_copies(chunk):
        slot = chunk % PAIR
        zt = chunk % Z_SIZE
        k = chunk // Z_SIZE
        copies = []
        for b in range(Z_SIZE):
            off = pl.multiple_of(384 * (Z_SIZE * zt + b) + LANES * k, LANES)
            copies.append(pltpu.make_async_copy(z_hbm.at[:, pl.ds(off, LANES)], zbuf.at[slot, b], zsem.at[slot, b]))
            copies.append(pltpu.make_async_copy(w2_hbm.at[:, pl.ds(off, LANES)], w2c.at[slot, :, pl.ds(b * LANES, LANES)], wsem.at[slot, b]))
        return copies

    big[0].start()
    for copy in chunk_copies(0):
        copy.start()
    big[1].start()
    big[PAIR].start()
    qbuf[...] = jnp.zeros(qbuf.shape, f32)

    barrier = pltpu.get_barrier_semaphore()
    for peer in [core_peer, x_peer, y_peer, diag_peer] + z_peers:
        pl.semaphore_signal(barrier, inc=1, device_id=(peer,), device_id_type=MESH_ID)
    pl.semaphore_wait(barrier, 7)
    for copy in big:
        copy.wait()

    def remote(src, dst, ssem, rsem, peer):
        return pltpu.make_async_remote_copy(src_ref=src, dst_ref=dst, send_sem=ssem, recv_sem=rsem, device_id=(peer,), device_id_type=MESH_ID)

    def pair0(chunk):
        slot = chunk % PAIR
        ring = chunk % ACC_SLOTS
        land = chunk % Z_SIZE
        return (remote(acc1.at[ring, 1 - core], ra0.at[land], sa_send.at[0, slot], sa_recv.at[0, land], core_peer),
                remote(acc2.at[ring, :, :, 1 - core], rb0.at[land], sb_send.at[0, slot], sb_recv.at[0, land], core_peer))

    def pair1(chunk):
        slot = chunk % PAIR
        land = chunk % Z_SIZE
        return (remote(s1a.at[slot, :, :, 1 - y_pos], ra1.at[land], sa_send.at[1, slot], sa_recv.at[1, land], y_peer),
                remote(s1b.at[slot, :, 1 - x_pos], rb1.at[land], sb_send.at[1, slot], sb_recv.at[1, land], x_peer))

    def pair2(chunk):
        slot = chunk % PAIR
        land = chunk % Z_SIZE
        return (remote(s2a.at[slot, 1 - x_pos], ra2.at[land], sa_send.at[PAIR, slot], sa_recv.at[PAIR, land], x_peer),
                remote(s2b.at[slot, 1 - y_pos], rb2.at[land], sb_send.at[PAIR, slot], sb_recv.at[PAIR, land], y_peer))

    def z_send_a(chunk):
        slot = chunk % PAIR
        land = chunk % Z_SIZE
        return [remote(s3a.at[slot, z_others[k]], ra3.at[land, z_pos], za_send.at[slot, k], za_recv.at[land, z_pos], z_peers[k]) for k in range(Z_PEERS)]

    def z_recv_a(chunk):
        slot = chunk % PAIR
        land = chunk % Z_SIZE
        return [remote(s3a.at[slot, z_others[k]], ra3.at[land, z_others[k]], za_send.at[slot, k], za_recv.at[land, z_others[k]], z_peers[k]) for k in range(Z_PEERS)]

    def z_send_b(chunk):
        zt = chunk % Z_SIZE
        return remote(s3b.at[chunk % PAIR], rb3.at[chunk // Z_SIZE, z_pos], zb_send.at[chunk % PAIR], zb_recv.at[chunk // Z_SIZE, z_pos], device_of(core, x_pos, y_pos, zt))

    def z_recv_b(chunk):
        return [remote(s3b.at[chunk % PAIR], rb3.at[chunk // Z_SIZE, z_others[k]], zb_send.at[chunk % PAIR], zb_recv.at[chunk // Z_SIZE, z_others[k]], z_peers[k]) for k in range(Z_PEERS)]

    lane_me = core * PAIR + x_pos
    group = ((1 - core, x_pos, core_peer), (core, 1 - x_pos, x_peer), (1 - core, 1 - x_pos, diag_peer))

    def g_send(chunk):
        slot = chunk % PAIR
        return [remote(qbuf.at[slot, gx * PAIR + gc], out1.at[lane_me, chunk], ga_send.at[slot, i], ga_recv.at[i, chunk % Z_SIZE], peer) for i, (gc, gx, peer) in enumerate(group)]

    def g_recv(chunk):
        slot = chunk % PAIR
        return [remote(qbuf.at[slot, gx * PAIR + gc], out1.at[gc * PAIR + gx, chunk], ga_send.at[slot, i], ga_recv.at[i, chunk % Z_SIZE], peer) for i, (gc, gx, peer) in enumerate(group)]

    def within(t, lead):
        return jnp.logical_and(t >= lead, t < lead + CHUNKS)

    def elementwise(slot, r, a_buf, d_buf):
        rows = pl.ds(pl.multiple_of(r * TILE_R, TILE_R), TILE_R)
        back = lax.dot_general(dh[rows, :], w2c[slot], (((1,), (0,)), ((), ())), preferred_element_type=f32).astype(jnp.bfloat16)
        for b in range(Z_SIZE):
            cols = slice(b * LANES, (b + 1) * LANES)
            wide = zbuf[slot, b, rows, :].astype(f32)
            cdf = 0.5 * (1.0 + lax.erf(wide * INV_SQRT2))
            a_buf[:, cols] = (wide * cdf).astype(jnp.bfloat16)
            slope = cdf + wide * INV_SQRT2PI * jnp.exp(-0.5 * wide * wide)
            d_buf[:, cols] = (back[:, cols].astype(f32) * slope).astype(jnp.bfloat16)

    def accumulate(ring, r, a_buf, d_buf, first):
        rows = pl.ds(pl.multiple_of(r * TILE_R, TILE_R), TILE_R)
        part1 = jnp.dot(xt[:, rows], d_buf[...], preferred_element_type=f32)
        part2 = jnp.dot(dht[:, rows], a_buf[...], preferred_element_type=f32)
        for b in range(Z_SIZE):
            c1, x1 = b // PAIR, b % PAIR
            val1 = part1[:, b * LANES:(b + 1) * LANES].reshape(Z_SIZE, PAIR, GROUP_ROWS, LANES)
            val2 = part2[:, b * LANES:(b + 1) * LANES].reshape(PAIR, HALF_ROWS, LANES)
            if first:
                acc1[ring, c1, x1] = val1
                acc2[ring, b // PAIR, b % PAIR] = val2
            else:
                acc1[ring, c1, x1] = acc1[ring, c1, x1] + val1
                acc2[ring, b // PAIR, b % PAIR] = acc2[ring, b // PAIR, b % PAIR] + val2

    n_tiles = ROWS_DEV // TILE_R

    def compute(chunk):
        slot = chunk % PAIR
        ring = chunk % ACC_SLOTS
        for copy in chunk_copies(chunk):
            copy.wait()

        @pl.when(chunk + 1 < CHUNKS)
        def _():
            for copy in chunk_copies(chunk + 1):
                copy.start()

        elementwise(slot, 0, a_even, d_even)
        elementwise(slot, 1, a_odd, d_odd)
        accumulate(ring, 0, a_even, d_even, True)

        def body(i, carry):
            elementwise(slot, PAIR * i, a_even, d_even)
            accumulate(ring, PAIR * i - 1, a_odd, d_odd, False)
            elementwise(slot, PAIR * i + 1, a_odd, d_odd)
            accumulate(ring, PAIR * i, a_even, d_even, False)
            return carry

        lax.fori_loop(1, n_tiles // PAIR, body, 0)
        accumulate(ring, n_tiles - 1, a_odd, d_odd, False)

    def step(t, carry):
        @pl.when(within(t, 11))
        def _():
            for copy in g_send(t - 11):
                copy.wait_send()
            for copy in g_recv(t - 11):
                copy.wait_recv()

        @pl.when(within(t, 9))
        def _():
            chunk = t - 9
            slot = chunk % PAIR
            land = chunk % Z_SIZE
            zt = chunk % Z_SIZE
            for copy in z_send_a(chunk):
                copy.wait_send()
            for copy in z_recv_a(chunk):
                copy.wait_recv()
            full = s3a[slot, z_pos]
            for zo in z_others:
                full = full + ra3[land, zo]
            for o in range(Z_SIZE):
                qbuf[slot, o, 0:OWN_ROWS, :] = full[OWN_ROWS * o:OWN_ROWS * (o + 1), :]
            out1[lane_me, chunk] = qbuf[slot, x_pos * PAIR + core]

            @pl.when(z_pos == zt)
            def _():
                for copy in z_recv_b(chunk):
                    copy.wait_recv()
                k = chunk // Z_SIZE
                total = s3b[slot]
                for zo in z_others:
                    total = total + rb3[k, zo]
                own2[k] = total

            @pl.when(z_pos != zt)
            def _():
                z_send_b(chunk).wait_send()

        @pl.when(within(t, 7))
        def _():
            chunk = t - 7
            slot = chunk % PAIR
            land = chunk % Z_SIZE
            for copy in pair2(chunk):
                copy.wait()
            for z in range(Z_SIZE):
                s3a[slot, z] = s2a[slot, x_pos, z] + ra2[land, z]
            s3b[slot] = s2b[slot, y_pos] + rb2[land]

        @pl.when(within(t, 5))
        def _():
            chunk = t - 5
            slot = chunk % PAIR
            land = chunk % Z_SIZE
            for copy in pair1(chunk):
                copy.wait()
            for x in range(PAIR):
                for z in range(Z_SIZE):
                    s2a[slot, x, z] = s1a[slot, x, z, y_pos] + ra1[land, x, z]
            for y in range(PAIR):
                s2b[slot, y] = s1b[slot, y, x_pos] + rb1[land, y]

        @pl.when(within(t, Z_PEERS))
        def _():
            chunk = t - Z_PEERS
            slot = chunk % PAIR
            land = chunk % Z_SIZE
            ring = chunk % ACC_SLOTS
            for copy in pair0(chunk):
                copy.wait()
            for x in range(PAIR):
                s1a[slot, x] = acc1[ring, core, x] + ra0[land, x]
            for y in range(PAIR):
                for x in range(PAIR):
                    s1b[slot, y, x] = acc2[ring, y, x, core] + rb0[land, y, x]

        for lead, copies in ((1, pair0), (Z_PEERS, pair1), (5, pair2), (7, z_send_a), (9, g_send)):
            @pl.when(within(t, lead))
            def _(lead=lead, copies=copies):
                for copy in copies(t - lead):
                    copy.start()

        @pl.when(jnp.logical_and(within(t, 7), z_pos != (t + 1) % Z_SIZE))
        def _():
            z_send_b(t - 7).start()

        @pl.when(t < CHUNKS)
        def _():
            compute(t)

        return carry

    lax.fori_loop(0, CHUNKS + 11, step, 0)

    fixes = [remote(own2.at[1 - core + i], out2.at[i, core], fix_send.at[i], fix_recv.at[i], core_peer) for i in range(PAIR)]
    for copy in fixes:
        copy.start()
    for i in range(PAIR):
        out2[i, core] = own2[core + i]
    for i in range(PAIR):
        remote(own2.at[1 - core + i], out2.at[i, 1 - core], fix_send.at[i], fix_recv.at[i], core_peer).wait()


def scatter_call(z_one, dh_two, dh_two_t, x_t, w_two):
    f32 = jnp.float32
    bf16 = jnp.bfloat16
    hbm = pl.BlockSpec(memory_space=pl.ANY)
    vmem = pl.BlockSpec(memory_space=pltpu.VMEM)
    dma = pltpu.SemaphoreType.DMA
    buf = pltpu.VMEM
    return pl.pallas_call(
        scatter_kernel,
        out_shape=[jax.ShapeDtypeStruct((Z_SIZE, CHUNKS, PAD_ROWS, LANES), f32), jax.ShapeDtypeStruct((PAIR, PAIR, HALF_ROWS, LANES), f32)],
        in_specs=[hbm] * 5,
        out_specs=[vmem, vmem],
        scratch_shapes=[
            buf((ROWS_DEV, MODEL_DIM), bf16), buf((MODEL_DIM, ROWS_DEV), bf16), buf((MODEL_DIM, ROWS_DEV), bf16),
            buf((PAIR, Z_SIZE, ROWS_DEV, LANES), bf16), buf((PAIR, MODEL_DIM, CHUNK_W), bf16),
            buf((TILE_R, CHUNK_W), bf16), buf((TILE_R, CHUNK_W), bf16), buf((TILE_R, CHUNK_W), bf16), buf((TILE_R, CHUNK_W), bf16),
            buf((ACC_SLOTS, PAIR, PAIR, Z_SIZE, PAIR, GROUP_ROWS, LANES), f32), buf((ACC_SLOTS, PAIR, PAIR, PAIR, HALF_ROWS, LANES), f32),
            buf((Z_SIZE, PAIR, Z_SIZE, PAIR, GROUP_ROWS, LANES), f32), buf((Z_SIZE, PAIR, Z_SIZE, GROUP_ROWS, LANES), f32), buf((Z_SIZE, Z_SIZE, GROUP_ROWS, LANES), f32), buf((Z_SIZE, Z_SIZE, GROUP_ROWS, LANES), f32),
            buf((Z_SIZE, PAIR, PAIR, HALF_ROWS, LANES), f32), buf((Z_SIZE, PAIR, HALF_ROWS, LANES), f32), buf((Z_SIZE, HALF_ROWS, LANES), f32), buf((Z_PEERS, Z_SIZE, HALF_ROWS, LANES), f32),
            buf((PAIR, PAIR, Z_SIZE, PAIR, GROUP_ROWS, LANES), f32), buf((PAIR, PAIR, Z_SIZE, GROUP_ROWS, LANES), f32), buf((PAIR, Z_SIZE, GROUP_ROWS, LANES), f32),
            buf((PAIR, PAIR, PAIR, HALF_ROWS, LANES), f32), buf((PAIR, PAIR, HALF_ROWS, LANES), f32), buf((PAIR, HALF_ROWS, LANES), f32),
            buf((Z_PEERS, HALF_ROWS, LANES), f32), buf((PAIR, Z_SIZE, PAD_ROWS, LANES), f32),
            dma((Z_PEERS,)), dma((PAIR, Z_SIZE)), dma((PAIR, Z_SIZE)),
            dma((Z_PEERS, PAIR)), dma((Z_PEERS, Z_SIZE)), dma((Z_PEERS, PAIR)), dma((Z_PEERS, Z_SIZE)),
            dma((PAIR, Z_PEERS)), dma((Z_SIZE, Z_SIZE)), dma((PAIR,)), dma((Z_PEERS, Z_SIZE)),
            dma((PAIR, Z_PEERS)), dma((Z_PEERS, Z_SIZE)), dma((PAIR,)), dma((PAIR,)),
        ],
        compiler_params=pltpu.CompilerParams(collective_id=1, has_side_effects=True, vmem_limit_bytes=60 * 1024 * 1024),
        cost_estimate=pl.CostEstimate(flops=100_000_000_000, bytes_accessed=80_000_000, transcendentals=50_000_000),
        name='grad_scatter',
    )(z_one, dh_two, dh_two_t, x_t, w_two)


def forward_kernel(xt_ref, dyt_ref, w1, w2t, w3, w4t, z_out, dh_out, dht_out, g3_out, g4t_out,
                   h_acc, a_even, a_odd, h_t, x_own, dy_own):
    f32 = jnp.float32
    bf16 = jnp.bfloat16

    @pl.when(pl.program_id(0) == 0)
    def _():
        g3_out[...] = jnp.zeros(g3_out.shape, f32)
        g4t_out[...] = jnp.zeros(g4t_out.shape, f32)

    def hidden(c, a_buf):
        cols = pl.ds(pl.multiple_of(c * CHUNK_W, CHUNK_W), CHUNK_W)
        z_val = jnp.dot(x_own[...], w1[:, cols], preferred_element_type=f32).astype(bf16)
        z_out[:, cols] = z_val
        a_buf[...] = gelu_value(z_val).astype(bf16)

    def project(c, a_buf, first):
        cols = pl.ds(pl.multiple_of(c * CHUNK_W, CHUNK_W), CHUNK_W)
        part = lax.dot_general(a_buf[...], w2t[:, cols], (((1,), (1,)), ((), ())), preferred_element_type=f32)
        if first:
            h_acc[...] = part
        else:
            h_acc[...] = h_acc[...] + part

    x_own[...] = xt_ref[...].T
    dy_own[...] = dyt_ref[...].T
    hidden(0, a_even)
    hidden(1, a_odd)
    project(0, a_even, True)

    def body(i, carry):
        hidden(PAIR * i, a_even)
        project(PAIR * i - 1, a_odd, False)
        hidden(PAIR * i + 1, a_odd)
        project(PAIR * i, a_even, False)
        return carry

    lax.fori_loop(1, CHUNKS // PAIR, body, 0)
    project(CHUNKS - 1, a_odd, False)
    h_two = h_acc[...].astype(bf16)
    h_t[...] = h_two.T
    dh_sum = None
    for j in range(w3.shape[1] // CHUNK_W):
        cols = slice(j * CHUNK_W, (j + 1) * CHUNK_W)
        z_three = jnp.dot(h_two, w3[:, cols], preferred_element_type=f32).astype(bf16)
        wide = z_three.astype(f32)
        cdf = 0.5 * (1.0 + lax.erf(wide * INV_SQRT2))
        a_three = (wide * cdf).astype(bf16)
        slope = cdf + wide * INV_SQRT2PI * jnp.exp(-0.5 * wide * wide)
        da_three = jnp.dot(dy_own[...], w4t[:, cols], preferred_element_type=f32).astype(bf16)
        dz_three = (da_three.astype(f32) * slope).astype(bf16)
        g4t_out[:, cols] = g4t_out[:, cols] + jnp.dot(dyt_ref[...], a_three, preferred_element_type=f32)
        g3_out[:, cols] = g3_out[:, cols] + jnp.dot(h_t[...], dz_three, preferred_element_type=f32)
        part = lax.dot_general(dz_three, w3[:, cols], (((1,), (1,)), ((), ())), preferred_element_type=f32)
        dh_sum = part if dh_sum is None else dh_sum + part
    dh_two = dh_sum.astype(bf16)
    dh_out[...] = dh_two
    dht_out[...] = dh_two.T


def forward_call(x_t, dy_t, w_one, w_two_t, w_three, w_four_t):
    f32 = jnp.float32
    bf16 = jnp.bfloat16
    buf = pltpu.VMEM
    rows_in = pl.BlockSpec((TILE_R, MODEL_DIM), lambda i: (i, 0))
    cols_out = pl.BlockSpec((MODEL_DIM, TILE_R), lambda i: (0, i))
    whole = lambda a: pl.BlockSpec(a.shape, lambda i: (0, 0), pipeline_mode=pl.Buffered(1))
    small = jax.ShapeDtypeStruct((MODEL_DIM, FF_DIM), f32)
    tall = jax.ShapeDtypeStruct((ROWS_DEV, MODEL_DIM), bf16)
    flat = jax.ShapeDtypeStruct((MODEL_DIM, ROWS_DEV), bf16)
    return pl.pallas_call(
        forward_kernel,
        grid=(ROWS_DEV // TILE_R,),
        out_shape=[jax.ShapeDtypeStruct((ROWS_DEV, WIDE_DIM), bf16), tall, flat, small, small],
        in_specs=[cols_out, cols_out] + [whole(a) for a in (w_one, w_two_t, w_three, w_four_t)],
        out_specs=[pl.BlockSpec((TILE_R, WIDE_DIM), lambda i: (i, 0)), rows_in, cols_out, whole(small), whole(small)],
        scratch_shapes=[buf((TILE_R, MODEL_DIM), f32), buf((TILE_R, CHUNK_W), bf16), buf((TILE_R, CHUNK_W), bf16), buf((MODEL_DIM, TILE_R), bf16), buf((TILE_R, MODEL_DIM), bf16), buf((TILE_R, MODEL_DIM), bf16)],
        compiler_params=pltpu.CompilerParams(vmem_limit_bytes=60 * 1024 * 1024),
        cost_estimate=pl.CostEstimate(flops=100_000_000_000, bytes_accessed=100_000_000, transcendentals=50_000_000),
        name='forward_chain',
    )(x_t, dy_t, w_one, w_two_t, w_three, w_four_t)


def unpack_kernel(p_ref, q_ref, norm_ref, lr_ref, clip_ref, *refs):
    states, (w1_out, w2t_out, w3_out, w4t_out), outs, (wide, lane_buf) = refs[:16], refs[16:20], refs[20:32], refs[32:]
    owners = p_ref.shape[0]

    @pl.when(pl.program_id(0) == 0)
    def _():
        lr_val = lr_ref[0, 0]
        scale = jnp.minimum(1.0, clip_ref[0, 0] / (norm_ref[...] + NORM_EPS))[0:1, 0:1]
        for i in range(Z_SIZE):
            g_ref, p_in, m_in, v_in = states[i::Z_SIZE]
            p_out, m_out, v_out = outs[i::Z_SIZE]
            p_out[...], m_out[...], v_out[...] = adam_new(g_ref[...], p_in[...], m_in[...], v_in[...], scale, lr_val)

    tall = jnp.concatenate([q_ref[o, :TALL_ROWS, :] for o in range(owners)], axis=0)
    w2t_out[...] = tall.T
    short = jnp.concatenate([q_ref[o, TALL_ROWS:, :] for o in range(owners)], axis=0)
    w4t_out[...] = short.T
    for o in range(owners):
        wide[o] = p_ref[o].astype(jnp.float32)
    for w_out, base in ((w1_out, 0), (w3_out, W1_ROWS)):
        for j in range(w_out.shape[1] // LANES):
            for o in range(owners):
                lane_buf[j % PAIR, o * OWN_ROWS:(o + 1) * OWN_ROWS, :] = wide[o, base + j * OWN_ROWS:base + (j + 1) * OWN_ROWS, :]
            w_out[:, j * LANES:(j + 1) * LANES] = lane_buf[j % PAIR].astype(jnp.bfloat16)


def unpack_call(all_p, all_q, norm, learn_rate, clip_max, states):
    f32 = jnp.float32
    bf16 = jnp.bfloat16
    owners = 8
    steps = DP_SIZE // owners
    fixed = lambda a: pl.BlockSpec(a.shape, lambda i: (0, 0))
    smem = pl.BlockSpec(memory_space=pltpu.SMEM)
    olds = [jax.ShapeDtypeStruct(a.shape, f32) for a in states[Z_SIZE:]]
    rows_of = lambda width: pl.BlockSpec((MODEL_DIM // steps, width), lambda i: (i, 0))
    cols_of = lambda width: pl.BlockSpec((MODEL_DIM, width // steps), lambda i: (0, i))
    return pl.pallas_call(
        unpack_kernel,
        grid=(steps,),
        out_shape=[jax.ShapeDtypeStruct((MODEL_DIM, w), bf16) for w in (WIDE_DIM, WIDE_DIM, FF_DIM, FF_DIM)] + olds,
        in_specs=[pl.BlockSpec((owners, PACK_ROWS, LANES), lambda i: (i, 0, 0)), pl.BlockSpec((owners, STACK_ROWS, MODEL_DIM), lambda i: (i, 0, 0)), fixed(norm), smem, smem] + [fixed(a) for a in states],
        out_specs=[rows_of(WIDE_DIM), cols_of(WIDE_DIM), rows_of(FF_DIM), cols_of(FF_DIM)] + [fixed(a) for a in olds],
        scratch_shapes=[pltpu.VMEM((owners, PACK_ROWS, LANES), f32), pltpu.VMEM((PAIR, owners * OWN_ROWS, LANES), f32)],
        compiler_params=pltpu.CompilerParams(vmem_limit_bytes=60 * 1024 * 1024),
        name='unpack_weights',
    )(all_p, all_q, norm, learn_rate.reshape(1, 1), clip_max.reshape(1, 1), *states)


def solution(mesh):
    row_spec = P('dp', None)
    rep_spec = P()

    def per_device(x_rows, dy_rows, w_one, w_two, w_three, w_four, master_one, master_two, master_three, master_four, m_one, m_two, m_three, m_four, v_one, v_two, v_three, v_four, learn_rate, clip_max):
        x_t, w_two_t = x_rows.T, w_two.T
        z_one, dh_two, dh_two_t, g_three, g_four_t = forward_call(x_t, dy_rows.T, w_one, w_two_t, w_three, w_four.T)
        small = jnp.concatenate([g.reshape(DP_SIZE, W3_ROWS, LANES) for g in (g_three, g_four_t.T)], axis=1)
        small_sum = lax.psum_scatter(small, 'dp', scatter_dimension=0, tiled=True).reshape(PAIR, W3_ROWS, LANES)
        s_three = small_sum[0].reshape(OWN_ROWS, FF_DIM)
        s_four = small_sum[1].reshape(SHORT_ROWS, MODEL_DIM)
        sum_one, sum_two = scatter_call(z_one, dh_two, dh_two_t, x_t, w_two_t)
        s_one = sum_one.reshape(Z_SIZE, Z_PEERS, Z_SIZE, PAD_ROWS, LANES)[:, :, :, :OWN_ROWS].transpose(Z_PEERS, PAIR, 0, 1, Z_SIZE).reshape(OWN_ROWS, WIDE_DIM)
        flat_two = sum_two.transpose(1, PAIR, 0, Z_PEERS).reshape(MODEL_DIM, 256)
        s_two = lax.dynamic_slice_in_dim(flat_two, 64 * (lax.axis_index('dp') % PAIR), TALL_ROWS, axis=1).T
        states = (s_one, s_two, s_three, s_four, master_one, master_two, master_three, master_four, m_one, m_two, m_three, m_four, v_one, v_two, v_three, v_four)
        all_p, all_q, norm = update_call(states, learn_rate, clip_max)
        outs = unpack_call(all_p, all_q, norm, learn_rate, clip_max, states)
        return (outs[0], outs[1].T, outs[2], outs[3].T) + tuple(outs[Z_SIZE:]) + (norm[0, 0],)

    in_specs = (row_spec, row_spec) + (rep_spec,) * Z_SIZE + (row_spec,) * 12 + (rep_spec, rep_spec)
    out_specs = (rep_spec,) * Z_SIZE + (row_spec,) * 12 + (rep_spec,)
    return jax.shard_map(per_device, mesh=mesh, in_specs=in_specs, out_specs=out_specs, check_vma=False)
```

```python
import jax
import jax.numpy as jnp
from jax import lax
from jax.experimental import pallas as pl
from jax.experimental.pallas import tpu as pltpu
from jax.sharding import PartitionSpec as P

ADAM_STEP = 10
BETA_ONE = 0.9
BETA_TWO = 0.95
ADAM_EPS = 1e-8
NORM_EPS = 1e-6
BIAS_ONE = 1.0 - BETA_ONE ** ADAM_STEP
BIAS_TWO = 1.0 - BETA_TWO ** ADAM_STEP
INV_SQRT2 = 0.7071067811865476
INV_SQRT2PI = 0.3989422804014327
DP_SIZE = 32
MESH_ID = pl.DeviceIdType.MESH
W1_ROWS = 48 * 18
W3_ROWS = 12 * 18
PACK_ROWS = 1088
CHUNKS = 12
CHUNK_W = 512
ROWS_DEV = 4096
TILE_R = 512
LANES = 128
MODEL_DIM = 576
GROUP_ROWS = 72
HALF_ROWS = 288
OWN_ROWS = 18
Z_SIZE = 4
PAIR = 2
ACC_SLOTS = 3
Z_PEERS = 3
PAD_ROWS = 24
WIDE_DIM = 6144
FF_DIM = 1536
STACK_ROWS = 240
TALL_ROWS = 192
SHORT_ROWS = 48
SMALL_USED = W3_ROWS + 5 * SHORT_ROWS
SMALL_ROWS = 480


def gelu_value(pre_act):
    pre_wide = pre_act.astype(jnp.float32)
    return 0.5 * pre_wide * (1.0 + lax.erf(pre_wide * INV_SQRT2))


def device_of(core, x_pos, y_pos, z_pos):
    return ((z_pos * PAIR + y_pos) * PAIR + x_pos) * PAIR + core


def adam_new(g_val, p_val, m_val, v_val, s_val, lr_val):
    scaled = s_val * (g_val * (1.0 / DP_SIZE))
    mom_new = BETA_ONE * m_val + (1.0 - BETA_ONE) * scaled
    var_new = BETA_TWO * v_val + (1.0 - BETA_TWO) * scaled * scaled
    return p_val - lr_val * (mom_new / BIAS_ONE) / (jnp.sqrt(var_new / BIAS_TWO) + ADAM_EPS), mom_new, var_new


def update_kernel(*refs):
    sources, (lr_ref, clip_ref, all_p, all_q, norm_ref), locals_, rest = refs[:16], refs[16:21], refs[21:37], refs[37:]
    wide_p, own_p, own_q, norm_send, norm_recv, norm_ssem, norm_rsem, send_p, recv_p, send_q, recv_q, local_sem, load_sem = rest
    g1, g2, g3, g4, p1, p2, p3, p4, m1, m2, m3, m4, v1, v2, v3, v4 = locals_
    loads = [pltpu.make_async_copy(src, dst, load_sem.at[i]) for i, (src, dst) in enumerate(zip(sources, locals_))]
    for copy in loads:
        copy.start()
    me = lax.axis_index('dp')
    core = me % PAIR
    x_pos = (me // PAIR) % PAIR
    y_pos = (me // Z_SIZE) % PAIR
    z_pos = me // 8
    core_peer = device_of(1 - core, x_pos, y_pos, z_pos)
    x_peer = device_of(core, 1 - x_pos, y_pos, z_pos)
    y_peer = device_of(core, x_pos, 1 - y_pos, z_pos)
    z_others = [(z_pos + k) % Z_SIZE for k in (1, PAIR, Z_PEERS)]
    z_peers = [device_of(core, x_pos, y_pos, zo) for zo in z_others]

    barrier = pltpu.get_barrier_semaphore()
    for peer in [core_peer, x_peer, y_peer] + z_peers:
        pl.semaphore_signal(barrier, inc=1, device_id=(peer,), device_id_type=MESH_ID)
    pl.semaphore_wait(barrier, 6)

    for copy in loads:
        copy.wait()
    inv_dp = 1.0 / DP_SIZE
    total = jnp.zeros((1, LANES), jnp.float32)
    for g_ref in (g1, g3):
        for j in range(g_ref.shape[1] // LANES):
            g_val = g_ref[:, j * LANES:(j + 1) * LANES] * inv_dp
            total = total + jnp.sum(g_val * g_val, axis=0, keepdims=True)
    scal = jnp.sum(total)
    for g_ref in (g2, g4):
        g_val = g_ref[...] * inv_dp
        scal = scal + jnp.sum(g_val * g_val)
    part = jnp.full((8, LANES), scal, jnp.float32)
    for stage, peer in enumerate((core_peer, x_peer, y_peer)):
        norm_send[stage] = part
        copy = pltpu.make_async_remote_copy(src_ref=norm_send.at[stage], dst_ref=norm_recv.at[stage], send_sem=norm_ssem.at[stage], recv_sem=norm_rsem.at[stage], device_id=(peer,), device_id_type=MESH_ID)
        copy.start()
        copy.wait()
        part = part + norm_recv[stage]
    norm_send[Z_PEERS] = part
    norm_recv[Z_PEERS + z_pos] = part
    z_copies = []
    for k in range(Z_PEERS):
        z_copies.append(pltpu.make_async_remote_copy(src_ref=norm_send.at[Z_PEERS], dst_ref=norm_recv.at[Z_PEERS + z_pos], send_sem=norm_ssem.at[Z_PEERS + k], recv_sem=norm_rsem.at[Z_PEERS + z_pos], device_id=(z_peers[k],), device_id_type=MESH_ID))
        z_copies[-1].start()
    for k in range(Z_PEERS):
        pltpu.make_async_remote_copy(src_ref=norm_send.at[Z_PEERS], dst_ref=norm_recv.at[Z_PEERS + z_others[k]], send_sem=norm_ssem.at[Z_PEERS + k], recv_sem=norm_rsem.at[Z_PEERS + z_others[k]], device_id=(z_peers[k],), device_id_type=MESH_ID).wait_recv()
    for k in range(Z_PEERS):
        z_copies[k].wait_send()
    sq_all = ((norm_recv[Z_PEERS] + norm_recv[Z_SIZE]) + norm_recv[5]) + norm_recv[6]
    norm_val = jnp.sqrt(sq_all)
    norm_ref[...] = norm_val
    lr_val = lr_ref[0, 0]
    scale = jnp.minimum(1.0, clip_ref[0, 0] / (norm_val + NORM_EPS))[0:1, :]

    for base, (g_ref, p_ref, m_ref, v_ref) in ((0, (g1, p1, m1, v1)), (W1_ROWS, (g3, p3, m3, v3))):
        for j in range(g_ref.shape[1] // LANES):
            cols = slice(j * LANES, (j + 1) * LANES)
            p_new = adam_new(g_ref[:, cols], p_ref[:, cols], m_ref[:, cols], v_ref[:, cols], scale, lr_val)[0]
            wide_p[base + OWN_ROWS * j:base + OWN_ROWS * (j + 1), :] = p_new
    wide_p[W1_ROWS + W3_ROWS:, :] = jnp.zeros((PACK_ROWS - W1_ROWS - W3_ROWS, LANES), jnp.float32)
    own_p[...] = wide_p[...].astype(jnp.bfloat16)
    scale_one = scale[0:1, 0:1]
    for base, (g_ref, p_ref, m_ref, v_ref) in ((0, (g2, p2, m2, v2)), (TALL_ROWS, (g4, p4, m4, v4))):
        for r in range(g_ref.shape[0] // 16):
            rows = slice(r * 16, (r + 1) * 16)
            p_new = adam_new(g_ref[rows, :], p_ref[rows, :], m_ref[rows, :], v_ref[rows, :], scale_one, lr_val)[0]
            own_q[base + 16 * r:base + 16 * (r + 1), :] = p_new.astype(jnp.bfloat16)

    loc_p = pltpu.make_async_copy(own_p, all_p.at[me], local_sem.at[0])
    loc_q = pltpu.make_async_copy(own_q, all_q.at[me], local_sem.at[1])
    loc_p.start()
    loc_q.start()

    pending = []

    def send(buf, own, ssem, rsem, kind, slot, origin, peer, first):
        src = own if first else buf.at[origin]
        copy = pltpu.make_async_remote_copy(src_ref=src, dst_ref=buf.at[origin], send_sem=ssem.at[kind, slot], recv_sem=rsem.at[origin], device_id=(peer,), device_id_type=MESH_ID)
        copy.start()
        pending.append(copy)

    def arrive(buf, own, ssem, rsem, origin):
        pltpu.make_async_remote_copy(src_ref=own, dst_ref=buf.at[origin], send_sem=ssem.at[0, 0], recv_sem=rsem.at[origin], device_id=(core_peer,), device_id_type=MESH_ID).wait_recv()

    sets = ((all_p, own_p, send_p, recv_p, y_peer, x_peer, True), (all_q, own_q, send_q, recv_q, x_peer, y_peer, False))

    def origin_of(y_first, dz, da, db, dc=0):
        zo = (z_pos + dz) % Z_SIZE
        yo, xo = (da, db) if y_first else (db, da)
        return device_of((core + dc) % PAIR, (x_pos + xo) % PAIR, (y_pos + yo) % PAIR, zo)

    for buf, own, ssem, rsem, peer_a, peer_b, y_first in sets:
        send(buf, own, ssem, rsem, Z_PEERS, 0, me, peer_a, True)
        send(buf, own, ssem, rsem, Z_SIZE, 0, me, peer_b, True)
        for k in range(Z_PEERS):
            send(buf, own, ssem, rsem, k, 0, me, z_peers[k], True)
        send(buf, own, ssem, rsem, 5, 0, me, core_peer, True)
    steps = [(0, 1, 0)]
    for dz in (1, Z_PEERS, PAIR):
        steps += [(dz, 0, 0)]
    for dz in (1, Z_PEERS, PAIR):
        steps += [(dz, 1, 0)]
    for dz, da, _ in steps:
        for buf, own, ssem, rsem, peer_a, peer_b, y_first in sets:
            origin = origin_of(y_first, dz, da, 0)
            arrive(buf, own, ssem, rsem, origin)
            slot = dz * PAIR + da
            if da == 0:
                send(buf, own, ssem, rsem, Z_PEERS, dz, origin, peer_a, False)
            send(buf, own, ssem, rsem, Z_SIZE, slot, origin, peer_b, False)
            send(buf, own, ssem, rsem, 5, slot, origin, core_peer, False)
    for dz, da in [(0, 0), (0, 1), (1, 0), (Z_PEERS, 0), (PAIR, 0), (1, 1), (Z_PEERS, 1), (PAIR, 1)]:
        for buf, own, ssem, rsem, peer_a, peer_b, y_first in sets:
            origin = origin_of(y_first, dz, da, 1)
            arrive(buf, own, ssem, rsem, origin)
            send(buf, own, ssem, rsem, 5, 8 + dz * PAIR + da, origin, core_peer, False)
    for dz in range(Z_SIZE):
        for da in range(PAIR):
            for db in range(PAIR):
                for buf, own, ssem, rsem, peer_a, peer_b, y_first in sets:
                    arrive(buf, own, ssem, rsem, origin_of(y_first, dz, da, db, 1))
    for copy in pending:
        copy.wait_send()
    loc_p.wait()
    loc_q.wait()


def update_call(states, learn_rate, clip_max):
    f32 = jnp.float32
    bf16 = jnp.bfloat16
    dma = pltpu.SemaphoreType.DMA
    buf = pltpu.VMEM
    smem = pl.BlockSpec(memory_space=pltpu.SMEM)
    hbm = pl.BlockSpec(memory_space=pl.ANY)
    vmem = pl.BlockSpec(memory_space=pltpu.VMEM)
    kinds = 6
    return pl.pallas_call(
        update_kernel,
        out_shape=[jax.ShapeDtypeStruct((DP_SIZE, PACK_ROWS, LANES), bf16), jax.ShapeDtypeStruct((DP_SIZE, STACK_ROWS, MODEL_DIM), bf16), jax.ShapeDtypeStruct((8, LANES), f32)],
        in_specs=[hbm] * len(states) + [smem, smem],
        out_specs=[hbm, hbm, vmem],
        scratch_shapes=[buf(a.shape, f32) for a in states] + [
            buf((PACK_ROWS, LANES), f32), buf((PACK_ROWS, LANES), bf16), buf((STACK_ROWS, MODEL_DIM), bf16),
            buf((Z_SIZE, 8, LANES), f32), buf((7, 8, LANES), f32), dma((kinds,)), dma((7,)),
            dma((kinds, 16)), dma((DP_SIZE,)), dma((kinds, 16)), dma((DP_SIZE,)), dma((PAIR,)), dma((len(states),)),
        ],
        compiler_params=pltpu.CompilerParams(collective_id=0, has_side_effects=True, vmem_limit_bytes=60 * 1024 * 1024),
        name='adam_gather',
    )(*states, learn_rate.reshape(1, 1), clip_max.reshape(1, 1))


def scatter_kernel(z_hbm, dh_hbm, dht_hbm, xt_hbm, w2_hbm, out1, out2,
                   dh, dht, xt, zbuf, w2c, a_even, a_odd, d_even, d_odd, acc1, acc2,
                   ra0, ra1, ra2, ra3, rb0, rb1, rb2, rb3, s1a, s2a, s3a, s1b, s2b, s3b, own2, qbuf,
                   in_sem, zsem, wsem, sa_send, sa_recv, sb_send, sb_recv, za_send, za_recv, zb_send, zb_recv, ga_send, ga_recv, fix_send, fix_recv):
    f32 = jnp.float32
    me = lax.axis_index('dp')
    core = me % PAIR
    x_pos = (me // PAIR) % PAIR
    y_pos = (me // Z_SIZE) % PAIR
    z_pos = me // 8
    core_peer = device_of(1 - core, x_pos, y_pos, z_pos)
    x_peer = device_of(core, 1 - x_pos, y_pos, z_pos)
    y_peer = device_of(core, x_pos, 1 - y_pos, z_pos)
    diag_peer = device_of(1 - core, 1 - x_pos, y_pos, z_pos)
    z_others = [(z_pos + k) % Z_SIZE for k in (1, PAIR, Z_PEERS)]
    z_peers = [device_of(core, x_pos, y_pos, zo) for zo in z_others]

    big = [pltpu.make_async_copy(src, dst, in_sem.at[i]) for i, (src, dst) in enumerate(((dh_hbm, dh), (dht_hbm, dht), (xt_hbm, xt)))]

    def chunk_copies(chunk):
        slot = chunk % PAIR
        zt = chunk % Z_SIZE
        k = chunk // Z_SIZE
        copies = []
        for b in range(Z_SIZE):
            off = pl.multiple_of(384 * (Z_SIZE * zt + b) + LANES * k, LANES)
            copies.append(pltpu.make_async_copy(z_hbm.at[:, pl.ds(off, LANES)], zbuf.at[slot, b], zsem.at[slot, b]))
            copies.append(pltpu.make_async_copy(w2_hbm.at[:, pl.ds(off, LANES)], w2c.at[slot, :, pl.ds(b * LANES, LANES)], wsem.at[slot, b]))
        return copies

    big[0].start()
    for copy in chunk_copies(0):
        copy.start()
    big[1].start()
    big[PAIR].start()
    qbuf[...] = jnp.zeros(qbuf.shape, f32)

    barrier = pltpu.get_barrier_semaphore()
    for peer in [core_peer, x_peer, y_peer, diag_peer] + z_peers:
        pl.semaphore_signal(barrier, inc=1, device_id=(peer,), device_id_type=MESH_ID)
    pl.semaphore_wait(barrier, 7)
    for copy in big:
        copy.wait()

    def remote(src, dst, ssem, rsem, peer):
        return pltpu.make_async_remote_copy(src_ref=src, dst_ref=dst, send_sem=ssem, recv_sem=rsem, device_id=(peer,), device_id_type=MESH_ID)

    def pair0(chunk):
        slot = chunk % PAIR
        ring = chunk % ACC_SLOTS
        land = chunk % Z_SIZE
        return (remote(acc1.at[ring, 1 - core], ra0.at[land], sa_send.at[0, slot], sa_recv.at[0, land], core_peer),
                remote(acc2.at[ring, :, :, 1 - core], rb0.at[land], sb_send.at[0, slot], sb_recv.at[0, land], core_peer))

    def pair1(chunk):
        slot = chunk % PAIR
        land = chunk % Z_SIZE
        return (remote(s1a.at[slot, :, :, 1 - y_pos], ra1.at[land], sa_send.at[1, slot], sa_recv.at[1, land], y_peer),
                remote(s1b.at[slot, :, 1 - x_pos], rb1.at[land], sb_send.at[1, slot], sb_recv.at[1, land], x_peer))

    def pair2(chunk):
        slot = chunk % PAIR
        land = chunk % Z_SIZE
        return (remote(s2a.at[slot, 1 - x_pos], ra2.at[land], sa_send.at[PAIR, slot], sa_recv.at[PAIR, land], x_peer),
                remote(s2b.at[slot, 1 - y_pos], rb2.at[land], sb_send.at[PAIR, slot], sb_recv.at[PAIR, land], y_peer))

    def z_send_a(chunk):
        slot = chunk % PAIR
        land = chunk % Z_SIZE
        return [remote(s3a.at[slot, z_others[k]], ra3.at[land, z_pos], za_send.at[slot, k], za_recv.at[land, z_pos], z_peers[k]) for k in range(Z_PEERS)]

    def z_recv_a(chunk):
        slot = chunk % PAIR
        land = chunk % Z_SIZE
        return [remote(s3a.at[slot, z_others[k]], ra3.at[land, z_others[k]], za_send.at[slot, k], za_recv.at[land, z_others[k]], z_peers[k]) for k in range(Z_PEERS)]

    def z_send_b(chunk):
        zt = chunk % Z_SIZE
        return remote(s3b.at[chunk % PAIR], rb3.at[chunk // Z_SIZE, z_pos], zb_send.at[chunk % PAIR], zb_recv.at[chunk // Z_SIZE, z_pos], device_of(core, x_pos, y_pos, zt))

    def z_recv_b(chunk):
        return [remote(s3b.at[chunk % PAIR], rb3.at[chunk // Z_SIZE, z_others[k]], zb_send.at[chunk % PAIR], zb_recv.at[chunk // Z_SIZE, z_others[k]], z_peers[k]) for k in range(Z_PEERS)]

    lane_me = core * PAIR + x_pos
    group = ((1 - core, x_pos, core_peer), (core, 1 - x_pos, x_peer), (1 - core, 1 - x_pos, diag_peer))

    def g_send(chunk):
        slot = chunk % PAIR
        return [remote(qbuf.at[slot, gx * PAIR + gc], out1.at[lane_me, chunk], ga_send.at[slot, i], ga_recv.at[i, chunk % Z_SIZE], peer) for i, (gc, gx, peer) in enumerate(group)]

    def g_recv(chunk):
        slot = chunk % PAIR
        return [remote(qbuf.at[slot, gx * PAIR + gc], out1.at[gc * PAIR + gx, chunk], ga_send.at[slot, i], ga_recv.at[i, chunk % Z_SIZE], peer) for i, (gc, gx, peer) in enumerate(group)]

    def within(t, lead):
        return jnp.logical_and(t >= lead, t < lead + CHUNKS)

    def elementwise(slot, r, a_buf, d_buf):
        rows = pl.ds(pl.multiple_of(r * TILE_R, TILE_R), TILE_R)
        back = lax.dot_general(dh[rows, :], w2c[slot], (((1,), (0,)), ((), ())), preferred_element_type=f32).astype(jnp.bfloat16)
        for b in range(Z_SIZE):
            cols = slice(b * LANES, (b + 1) * LANES)
            wide = zbuf[slot, b, rows, :].astype(f32)
            cdf = 0.5 * (1.0 + lax.erf(wide * INV_SQRT2))
            a_buf[:, cols] = (wide * cdf).astype(jnp.bfloat16)
            slope = cdf + wide * INV_SQRT2PI * jnp.exp(-0.5 * wide * wide)
            d_buf[:, cols] = (back[:, cols].astype(f32) * slope).astype(jnp.bfloat16)

    def accumulate(ring, r, a_buf, d_buf, first):
        rows = pl.ds(pl.multiple_of(r * TILE_R, TILE_R), TILE_R)
        part1 = jnp.dot(xt[:, rows], d_buf[...], preferred_element_type=f32)
        part2 = jnp.dot(dht[:, rows], a_buf[...], preferred_element_type=f32)
        for b in range(Z_SIZE):
            c1, x1 = b // PAIR, b % PAIR
            val1 = part1[:, b * LANES:(b + 1) * LANES].reshape(Z_SIZE, PAIR, GROUP_ROWS, LANES)
            val2 = part2[:, b * LANES:(b + 1) * LANES].reshape(PAIR, HALF_ROWS, LANES)
            if first:
                acc1[ring, c1, x1] = val1
                acc2[ring, b // PAIR, b % PAIR] = val2
            else:
                acc1[ring, c1, x1] = acc1[ring, c1, x1] + val1
                acc2[ring, b // PAIR, b % PAIR] = acc2[ring, b // PAIR, b % PAIR] + val2

    n_tiles = ROWS_DEV // TILE_R

    def compute(chunk):
        slot = chunk % PAIR
        ring = chunk % ACC_SLOTS
        for copy in chunk_copies(chunk):
            copy.wait()

        @pl.when(chunk + 1 < CHUNKS)
        def _():
            for copy in chunk_copies(chunk + 1):
                copy.start()

        elementwise(slot, 0, a_even, d_even)
        elementwise(slot, 1, a_odd, d_odd)
        accumulate(ring, 0, a_even, d_even, True)

        def body(i, carry):
            elementwise(slot, PAIR * i, a_even, d_even)
            accumulate(ring, PAIR * i - 1, a_odd, d_odd, False)
            elementwise(slot, PAIR * i + 1, a_odd, d_odd)
            accumulate(ring, PAIR * i, a_even, d_even, False)
            return carry

        lax.fori_loop(1, n_tiles // PAIR, body, 0)
        accumulate(ring, n_tiles - 1, a_odd, d_odd, False)

    def step(t, carry):
        @pl.when(within(t, 11))
        def _():
            for copy in g_send(t - 11):
                copy.wait_send()
            for copy in g_recv(t - 11):
                copy.wait_recv()

        @pl.when(within(t, 9))
        def _():
            chunk = t - 9
            slot = chunk % PAIR
            land = chunk % Z_SIZE
            zt = chunk % Z_SIZE
            for copy in z_send_a(chunk):
                copy.wait_send()
            for copy in z_recv_a(chunk):
                copy.wait_recv()
            full = s3a[slot, z_pos]
            for zo in z_others:
                full = full + ra3[land, zo]
            for o in range(Z_SIZE):
                qbuf[slot, o, 0:OWN_ROWS, :] = full[OWN_ROWS * o:OWN_ROWS * (o + 1), :]
            out1[lane_me, chunk] = qbuf[slot, x_pos * PAIR + core]

            @pl.when(z_pos == zt)
            def _():
                for copy in z_recv_b(chunk):
                    copy.wait_recv()
                k = chunk // Z_SIZE
                total = s3b[slot]
                for zo in z_others:
                    total = total + rb3[k, zo]
                own2[k] = total

            @pl.when(z_pos != zt)
            def _():
                z_send_b(chunk).wait_send()

        @pl.when(within(t, 7))
        def _():
            chunk = t - 7
            slot = chunk % PAIR
            land = chunk % Z_SIZE
            for copy in pair2(chunk):
                copy.wait()
            for z in range(Z_SIZE):
                s3a[slot, z] = s2a[slot, x_pos, z] + ra2[land, z]
            s3b[slot] = s2b[slot, y_pos] + rb2[land]

        @pl.when(within(t, 5))
        def _():
            chunk = t - 5
            slot = chunk % PAIR
            land = chunk % Z_SIZE
            for copy in pair1(chunk):
                copy.wait()
            for x in range(PAIR):
                for z in range(Z_SIZE):
                    s2a[slot, x, z] = s1a[slot, x, z, y_pos] + ra1[land, x, z]
            for y in range(PAIR):
                s2b[slot, y] = s1b[slot, y, x_pos] + rb1[land, y]

        @pl.when(within(t, Z_PEERS))
        def _():
            chunk = t - Z_PEERS
            slot = chunk % PAIR
            land = chunk % Z_SIZE
            ring = chunk % ACC_SLOTS
            for copy in pair0(chunk):
                copy.wait()
            for x in range(PAIR):
                s1a[slot, x] = acc1[ring, core, x] + ra0[land, x]
            for y in range(PAIR):
                for x in range(PAIR):
                    s1b[slot, y, x] = acc2[ring, y, x, core] + rb0[land, y, x]

        for lead, copies in ((1, pair0), (Z_PEERS, pair1), (5, pair2), (7, z_send_a), (9, g_send)):
            @pl.when(within(t, lead))
            def _(lead=lead, copies=copies):
                for copy in copies(t - lead):
                    copy.start()

        @pl.when(jnp.logical_and(within(t, 7), z_pos != (t + 1) % Z_SIZE))
        def _():
            z_send_b(t - 7).start()

        @pl.when(t < CHUNKS)
        def _():
            compute(t)

        return carry

    lax.fori_loop(0, CHUNKS + 11, step, 0)

    fixes = [remote(own2.at[1 - core + i], out2.at[i, core], fix_send.at[i], fix_recv.at[i], core_peer) for i in range(PAIR)]
    for copy in fixes:
        copy.start()
    for i in range(PAIR):
        out2[i, core] = own2[core + i]
    for i in range(PAIR):
        remote(own2.at[1 - core + i], out2.at[i, 1 - core], fix_send.at[i], fix_recv.at[i], core_peer).wait()


def scatter_call(z_one, dh_two, dh_two_t, x_t, w_two):
    f32 = jnp.float32
    bf16 = jnp.bfloat16
    hbm = pl.BlockSpec(memory_space=pl.ANY)
    vmem = pl.BlockSpec(memory_space=pltpu.VMEM)
    dma = pltpu.SemaphoreType.DMA
    buf = pltpu.VMEM
    return pl.pallas_call(
        scatter_kernel,
        out_shape=[jax.ShapeDtypeStruct((Z_SIZE, CHUNKS, PAD_ROWS, LANES), f32), jax.ShapeDtypeStruct((PAIR, PAIR, HALF_ROWS, LANES), f32)],
        in_specs=[hbm] * 5,
        out_specs=[vmem, vmem],
        scratch_shapes=[
            buf((ROWS_DEV, MODEL_DIM), bf16), buf((MODEL_DIM, ROWS_DEV), bf16), buf((MODEL_DIM, ROWS_DEV), bf16),
            buf((PAIR, Z_SIZE, ROWS_DEV, LANES), bf16), buf((PAIR, MODEL_DIM, CHUNK_W), bf16),
            buf((TILE_R, CHUNK_W), bf16), buf((TILE_R, CHUNK_W), bf16), buf((TILE_R, CHUNK_W), bf16), buf((TILE_R, CHUNK_W), bf16),
            buf((ACC_SLOTS, PAIR, PAIR, Z_SIZE, PAIR, GROUP_ROWS, LANES), f32), buf((ACC_SLOTS, PAIR, PAIR, PAIR, HALF_ROWS, LANES), f32),
            buf((Z_SIZE, PAIR, Z_SIZE, PAIR, GROUP_ROWS, LANES), f32), buf((Z_SIZE, PAIR, Z_SIZE, GROUP_ROWS, LANES), f32), buf((Z_SIZE, Z_SIZE, GROUP_ROWS, LANES), f32), buf((Z_SIZE, Z_SIZE, GROUP_ROWS, LANES), f32),
            buf((Z_SIZE, PAIR, PAIR, HALF_ROWS, LANES), f32), buf((Z_SIZE, PAIR, HALF_ROWS, LANES), f32), buf((Z_SIZE, HALF_ROWS, LANES), f32), buf((Z_PEERS, Z_SIZE, HALF_ROWS, LANES), f32),
            buf((PAIR, PAIR, Z_SIZE, PAIR, GROUP_ROWS, LANES), f32), buf((PAIR, PAIR, Z_SIZE, GROUP_ROWS, LANES), f32), buf((PAIR, Z_SIZE, GROUP_ROWS, LANES), f32),
            buf((PAIR, PAIR, PAIR, HALF_ROWS, LANES), f32), buf((PAIR, PAIR, HALF_ROWS, LANES), f32), buf((PAIR, HALF_ROWS, LANES), f32),
            buf((Z_PEERS, HALF_ROWS, LANES), f32), buf((PAIR, Z_SIZE, PAD_ROWS, LANES), f32),
            dma((Z_PEERS,)), dma((PAIR, Z_SIZE)), dma((PAIR, Z_SIZE)),
            dma((Z_PEERS, PAIR)), dma((Z_PEERS, Z_SIZE)), dma((Z_PEERS, PAIR)), dma((Z_PEERS, Z_SIZE)),
            dma((PAIR, Z_PEERS)), dma((Z_SIZE, Z_SIZE)), dma((PAIR,)), dma((Z_PEERS, Z_SIZE)),
            dma((PAIR, Z_PEERS)), dma((Z_PEERS, Z_SIZE)), dma((PAIR,)), dma((PAIR,)),
        ],
        compiler_params=pltpu.CompilerParams(collective_id=1, has_side_effects=True, vmem_limit_bytes=60 * 1024 * 1024),
        cost_estimate=pl.CostEstimate(flops=100_000_000_000, bytes_accessed=80_000_000, transcendentals=50_000_000),
        name='grad_scatter',
    )(z_one, dh_two, dh_two_t, x_t, w_two)


def forward_kernel(xt_ref, dyt_ref, w1, w2t, w3, w4t, z_out, dh_out, dht_out, small_out,
                   g3_out, g4t_out, h_acc, a_even, a_odd, h_t, x_own, dy_own):
    f32 = jnp.float32
    bf16 = jnp.bfloat16

    @pl.when(pl.program_id(0) == 0)
    def _():
        g3_out[...] = jnp.zeros(g3_out.shape, f32)
        g4t_out[...] = jnp.zeros(g4t_out.shape, f32)

    def hidden(c, a_buf):
        cols = pl.ds(pl.multiple_of(c * CHUNK_W, CHUNK_W), CHUNK_W)
        z_val = jnp.dot(x_own[...], w1[:, cols], preferred_element_type=f32).astype(bf16)
        z_out[:, cols] = z_val
        a_buf[...] = gelu_value(z_val).astype(bf16)

    def project(c, a_buf, first):
        cols = pl.ds(pl.multiple_of(c * CHUNK_W, CHUNK_W), CHUNK_W)
        part = lax.dot_general(a_buf[...], w2t[:, cols], (((1,), (1,)), ((), ())), preferred_element_type=f32)
        if first:
            h_acc[...] = part
        else:
            h_acc[...] = h_acc[...] + part

    x_own[...] = xt_ref[...].T
    dy_own[...] = dyt_ref[...].T
    hidden(0, a_even)
    hidden(1, a_odd)
    project(0, a_even, True)

    def body(i, carry):
        hidden(PAIR * i, a_even)
        project(PAIR * i - 1, a_odd, False)
        hidden(PAIR * i + 1, a_odd)
        project(PAIR * i, a_even, False)
        return carry

    lax.fori_loop(1, CHUNKS // PAIR, body, 0)
    project(CHUNKS - 1, a_odd, False)
    h_two = h_acc[...].astype(bf16)
    h_t[...] = h_two.T
    dh_sum = None
    for j in range(w3.shape[1] // CHUNK_W):
        cols = slice(j * CHUNK_W, (j + 1) * CHUNK_W)
        z_three = jnp.dot(h_two, w3[:, cols], preferred_element_type=f32).astype(bf16)
        wide = z_three.astype(f32)
        cdf = 0.5 * (1.0 + lax.erf(wide * INV_SQRT2))
        a_three = (wide * cdf).astype(bf16)
        slope = cdf + wide * INV_SQRT2PI * jnp.exp(-0.5 * wide * wide)
        da_three = jnp.dot(dy_own[...], w4t[:, cols], preferred_element_type=f32).astype(bf16)
        dz_three = (da_three.astype(f32) * slope).astype(bf16)
        g4t_out[:, cols] = g4t_out[:, cols] + jnp.dot(dyt_ref[...], a_three, preferred_element_type=f32)
        g3_out[:, cols] = g3_out[:, cols] + jnp.dot(h_t[...], dz_three, preferred_element_type=f32)
        part = lax.dot_general(dz_three, w3[:, cols], (((1,), (1,)), ((), ())), preferred_element_type=f32)
        dh_sum = part if dh_sum is None else dh_sum + part
    dh_two = dh_sum.astype(bf16)
    dh_out[...] = dh_two
    dht_out[...] = dh_two.T

    @pl.when(pl.program_id(0) == ROWS_DEV // TILE_R - 1)
    def _():
        for d in range(DP_SIZE):
            for j in range(CHUNKS):
                small_out[d, j * OWN_ROWS:(j + 1) * OWN_ROWS, :] = g3_out[d * OWN_ROWS:(d + 1) * OWN_ROWS, j * LANES:(j + 1) * LANES]
        small_out[:, SMALL_USED:, :] = jnp.zeros((DP_SIZE, SMALL_ROWS - SMALL_USED, LANES), f32)
        whole_lanes = MODEL_DIM // LANES
        rest = MODEL_DIM - whole_lanes * LANES
        group = 8
        for e in range(DP_SIZE // group):
            turned = g4t_out[:, e * group * SHORT_ROWS:(e + 1) * group * SHORT_ROWS].T
            for i in range(group):
                rows = turned[i * SHORT_ROWS:(i + 1) * SHORT_ROWS, :]
                for j in range(whole_lanes):
                    small_out[e * group + i, W3_ROWS + j * SHORT_ROWS:W3_ROWS + (j + 1) * SHORT_ROWS, :] = rows[:, j * LANES:(j + 1) * LANES]
                last = W3_ROWS + whole_lanes * SHORT_ROWS
                small_out[e * group + i, last:SMALL_USED, :] = jnp.concatenate([rows[:, whole_lanes * LANES:], jnp.zeros((SHORT_ROWS, LANES - rest), f32)], axis=1)


def forward_call(x_t, dy_t, w_one, w_two_t, w_three, w_four_t):
    f32 = jnp.float32
    bf16 = jnp.bfloat16
    buf = pltpu.VMEM
    rows_in = pl.BlockSpec((TILE_R, MODEL_DIM), lambda i: (i, 0))
    cols_out = pl.BlockSpec((MODEL_DIM, TILE_R), lambda i: (0, i))
    whole = lambda a: pl.BlockSpec(a.shape, lambda i: (0, 0), pipeline_mode=pl.Buffered(1))
    small = jax.ShapeDtypeStruct((DP_SIZE, SMALL_ROWS, LANES), f32)
    tall = jax.ShapeDtypeStruct((ROWS_DEV, MODEL_DIM), bf16)
    flat = jax.ShapeDtypeStruct((MODEL_DIM, ROWS_DEV), bf16)
    return pl.pallas_call(
        forward_kernel,
        grid=(ROWS_DEV // TILE_R,),
        out_shape=[jax.ShapeDtypeStruct((ROWS_DEV, WIDE_DIM), bf16), tall, flat, small],
        in_specs=[cols_out, cols_out] + [whole(a) for a in (w_one, w_two_t, w_three, w_four_t)],
        out_specs=[pl.BlockSpec((TILE_R, WIDE_DIM), lambda i: (i, 0)), rows_in, cols_out, pl.BlockSpec(small.shape, lambda i: (0, 0, 0), pipeline_mode=pl.Buffered(1))],
        scratch_shapes=[buf((MODEL_DIM, FF_DIM), f32), buf((MODEL_DIM, FF_DIM), f32), buf((TILE_R, MODEL_DIM), f32), buf((TILE_R, CHUNK_W), bf16), buf((TILE_R, CHUNK_W), bf16), buf((MODEL_DIM, TILE_R), bf16), buf((TILE_R, MODEL_DIM), bf16), buf((TILE_R, MODEL_DIM), bf16)],
        compiler_params=pltpu.CompilerParams(vmem_limit_bytes=60 * 1024 * 1024),
        cost_estimate=pl.CostEstimate(flops=100_000_000_000, bytes_accessed=100_000_000, transcendentals=50_000_000),
        name='forward_chain',
    )(x_t, dy_t, w_one, w_two_t, w_three, w_four_t)


def unpack_kernel(p_ref, q_ref, norm_ref, lr_ref, clip_ref, *refs):
    states, (w1_out, w2t_out, w3_out, w4t_out), outs, (wide, lane_buf) = refs[:16], refs[16:20], refs[20:32], refs[32:]
    owners = p_ref.shape[0]

    @pl.when(pl.program_id(0) == 0)
    def _():
        lr_val = lr_ref[0, 0]
        scale = jnp.minimum(1.0, clip_ref[0, 0] / (norm_ref[...] + NORM_EPS))[0:1, 0:1]
        for i in range(Z_SIZE):
            g_ref, p_in, m_in, v_in = states[i::Z_SIZE]
            p_out, m_out, v_out = outs[i::Z_SIZE]
            p_out[...], m_out[...], v_out[...] = adam_new(g_ref[...], p_in[...], m_in[...], v_in[...], scale, lr_val)

    tall = jnp.concatenate([q_ref[o, :TALL_ROWS, :] for o in range(owners)], axis=0)
    w2t_out[...] = tall.T
    short = jnp.concatenate([q_ref[o, TALL_ROWS:, :] for o in range(owners)], axis=0)
    w4t_out[...] = short.T
    for o in range(owners):
        wide[o] = p_ref[o].astype(jnp.float32)
    for w_out, base in ((w1_out, 0), (w3_out, W1_ROWS)):
        for j in range(w_out.shape[1] // LANES):
            for o in range(owners):
                lane_buf[j % PAIR, o * OWN_ROWS:(o + 1) * OWN_ROWS, :] = wide[o, base + j * OWN_ROWS:base + (j + 1) * OWN_ROWS, :]
            w_out[:, j * LANES:(j + 1) * LANES] = lane_buf[j % PAIR].astype(jnp.bfloat16)


def unpack_call(all_p, all_q, norm, learn_rate, clip_max, states):
    f32 = jnp.float32
    bf16 = jnp.bfloat16
    owners = 8
    steps = DP_SIZE // owners
    fixed = lambda a: pl.BlockSpec(a.shape, lambda i: (0, 0))
    smem = pl.BlockSpec(memory_space=pltpu.SMEM)
    olds = [jax.ShapeDtypeStruct(a.shape, f32) for a in states[Z_SIZE:]]
    rows_of = lambda width: pl.BlockSpec((MODEL_DIM // steps, width), lambda i: (i, 0))
    cols_of = lambda width: pl.BlockSpec((MODEL_DIM, width // steps), lambda i: (0, i))
    return pl.pallas_call(
        unpack_kernel,
        grid=(steps,),
        out_shape=[jax.ShapeDtypeStruct((MODEL_DIM, w), bf16) for w in (WIDE_DIM, WIDE_DIM, FF_DIM, FF_DIM)] + olds,
        in_specs=[pl.BlockSpec((owners, PACK_ROWS, LANES), lambda i: (i, 0, 0)), pl.BlockSpec((owners, STACK_ROWS, MODEL_DIM), lambda i: (i, 0, 0)), fixed(norm), smem, smem] + [fixed(a) for a in states],
        out_specs=[rows_of(WIDE_DIM), cols_of(WIDE_DIM), rows_of(FF_DIM), cols_of(FF_DIM)] + [fixed(a) for a in olds],
        scratch_shapes=[pltpu.VMEM((owners, PACK_ROWS, LANES), f32), pltpu.VMEM((PAIR, owners * OWN_ROWS, LANES), f32)],
        compiler_params=pltpu.CompilerParams(vmem_limit_bytes=60 * 1024 * 1024),
        name='unpack_weights',
    )(all_p, all_q, norm, learn_rate.reshape(1, 1), clip_max.reshape(1, 1), *states)


def solution(mesh):
    row_spec = P('dp', None)
    rep_spec = P()

    def per_device(x_rows, dy_rows, w_one, w_two, w_three, w_four, master_one, master_two, master_three, master_four, m_one, m_two, m_three, m_four, v_one, v_two, v_three, v_four, learn_rate, clip_max):
        x_t, w_two_t = x_rows.T, w_two.T
        z_one, dh_two, dh_two_t, small = forward_call(x_t, dy_rows.T, w_one, w_two_t, w_three, w_four.T)
        small_sum = lax.psum_scatter(small.reshape(-1, LANES), 'dp', scatter_dimension=0, tiled=True)
        s_three = small_sum[:W3_ROWS].reshape(CHUNKS, OWN_ROWS, LANES).transpose(1, 0, 2).reshape(OWN_ROWS, FF_DIM)
        s_four = small_sum[W3_ROWS:SMALL_USED].reshape(5, SHORT_ROWS, LANES).transpose(1, 0, 2).reshape(SHORT_ROWS, 5 * LANES)[:, :MODEL_DIM]
        sum_one, sum_two = scatter_call(z_one, dh_two, dh_two_t, x_t, w_two_t)
        s_one = sum_one.reshape(Z_SIZE, Z_PEERS, Z_SIZE, PAD_ROWS, LANES)[:, :, :, :OWN_ROWS].transpose(Z_PEERS, PAIR, 0, 1, Z_SIZE).reshape(OWN_ROWS, WIDE_DIM)
        flat_two = sum_two.transpose(1, PAIR, 0, Z_PEERS).reshape(MODEL_DIM, 256)
        s_two = lax.dynamic_slice_in_dim(flat_two, 64 * (lax.axis_index('dp') % PAIR), TALL_ROWS, axis=1).T
        states = (s_one, s_two, s_three, s_four, master_one, master_two, master_three, master_four, m_one, m_two, m_three, m_four, v_one, v_two, v_three, v_four)
        all_p, all_q, norm = update_call(states, learn_rate, clip_max)
        outs = unpack_call(all_p, all_q, norm, learn_rate, clip_max, states)
        return (outs[0], outs[1].T, outs[2], outs[3].T) + tuple(outs[Z_SIZE:]) + (norm[0, 0],)

    in_specs = (row_spec, row_spec) + (rep_spec,) * Z_SIZE + (row_spec,) * 12 + (rep_spec, rep_spec)
    out_specs = (rep_spec,) * Z_SIZE + (row_spec,) * 12 + (rep_spec,)
    return jax.shard_map(per_device, mesh=mesh, in_specs=in_specs, out_specs=out_specs, check_vma=False)
```
